32 devices in a mesh: slices: 2 (over x), wide: 4 (over y, core), narrow: 4 (over z).
Axes of the slice: x: 2, y: 2, z: 4, core: 2. Of those that a mesh axis runs over, the one named last changes fastest.
Arguments:
- state: float32 [8, 4, 2, 16384], P(('slices', 'wide'), 'narrow'), parts along dimension 0, may hold values from -6 to 6
- gates: float32 [8, 7, 2, 4, 4], replicated, may hold values from -2 to 2
Outputs:
- final_state: float32 [8, 4, 2, 16384], P(('slices', 'wide'), 'narrow'), parts along dimension 0
- marginal: float32 [8, 16384], P(('slices', 'wide'), 'narrow'), parts along dimension 0
The draws below stay inside these ranges and needn't reach their ends.
There are 2 independent parts, one for each index of `slices`. The reference program is written for one: setup_inputs(seed, part) draws one part's arguments, and reference() takes and returns one part's arrays. A program takes and returns all parts, laid end to end along the dimension named above; an argument that names none is the same for every part. Nothing has to cross between parts.
All inputs are finite; a program needn't handle non-finite values.
Results may differ from the reference program's by a relative error of at most 0.0003.
Values sent between devices are 32-bit elements; how exact they have to be, the bound alone decides.
A program may use at most 192 MiB of HBM per device.

```python
import jax
import jax.numpy as jnp
from jax import lax

LAYERS = 8
AMP_DEV = 16384
PAIRS = 7
N_WIDE = 4
N_NARROW = 4


def steps_of(stream_key, dims, shards, low, largest):
    factor_of, own = 1.0, jax.random.fold_in(stream_key, 6)
    for axis_at, blocks in shards:
        heights = jnp.exp(jax.random.uniform(jax.random.fold_in(own, axis_at), (blocks,), jnp.float32, low / len(shards), largest / len(shards)))
        factor_of = factor_of * jnp.repeat(heights, dims[axis_at] // blocks).reshape([-1 if axis == axis_at else 1 for axis in range(len(dims))])
    return factor_of


def noise(stream_key, dims, deviation, most, shards=(), kind=jnp.bfloat16):
    drawn = deviation * jax.random.normal(stream_key, dims, jnp.float32)
    if shards:
        drawn = drawn * steps_of(stream_key, dims, shards, -0.22, 0.18)
    return jnp.clip(drawn, -most, most).astype(kind)


def setup_inputs(seed: int = 0, part: int = 0) -> dict:
    key_list = jax.random.split(jax.random.key(seed), 3)
    part_keys = jax.random.split(jax.random.fold_in(key_list[2], part), 3)
    state = noise(part_keys[0], (N_WIDE, N_NARROW, 2, AMP_DEV), 1.0, 6.0, ((0, 4), (1, 4)), jnp.float32)
    gates = noise(key_list[1], (LAYERS, PAIRS, 2, 4, 4), 8 ** -0.5, 2.0, (), jnp.float32)
    return {"state": state, "gates": gates}


BIT_LETTERS = "abdefghjklmnpqrstuvwxyzABCDEFGHIJKLM"


def apply_gate(psi, gate, low_label, high_label, total_bits):
    letters = BIT_LETTERS[:total_bits]
    low_pos = total_bits - 1 - low_label
    high_pos = total_bits - 1 - high_label
    source = "i" + letters
    target_list = list(letters)
    target_list[high_pos] = "W"
    target_list[low_pos] = "X"
    target = "o" + "".join(target_list)
    real_part = gate[0]
    imag_part = gate[1]
    block = jnp.stack([jnp.stack([real_part, -imag_part]), jnp.stack([imag_part, real_part])])
    block = block.reshape(2, 2, 2, 2, 2, 2)
    gate_form = "oiWX" + letters[high_pos] + letters[low_pos]
    return jnp.einsum(gate_form + "," + source + "->" + target, block, psi, precision=lax.Precision.HIGHEST)


def reference(state, gates):
    high_bits = (N_WIDE * N_NARROW).bit_length() - 1
    local_bits = AMP_DEV.bit_length() - 1
    total_bits = local_bits + high_bits
    psi = jnp.transpose(state, (2, 0, 1, 3)).reshape((2,) + (2,) * total_bits)
    for layer_index in range(LAYERS):
        start = layer_index * high_bits
        for pair_index in range(local_bits // 2):
            low_label = (start + 2 * pair_index) % total_bits
            high_label = (start + 2 * pair_index + 1) % total_bits
            psi = apply_gate(psi, gates[layer_index, pair_index], low_label, high_label, total_bits)
    offset = ((LAYERS - 1) * high_bits) % total_bits
    axes_order = [0] + [1 + total_bits - 1 - ((offset + place) % total_bits) for place in range(total_bits - 1, -1, -1)]
    final = jnp.transpose(psi, axes_order).reshape(2, N_WIDE, N_NARROW, AMP_DEV)
    prob = final[0] * final[0] + final[1] * final[1]
    marginal = jnp.sum(prob, axis=1)
    return jnp.transpose(final, (1, 2, 0, 3)), marginal
```

```python
import functools

import jax
import jax.numpy as jnp
from jax import lax
from jax.experimental import pallas as pl
from jax.experimental.pallas import tpu as pltpu
from jax.sharding import PartitionSpec as P


def kron_chain(members):
    real_part = members[0][0]
    imag_part = members[0][1]
    for member in members[1:]:
        other_real = member[0]
        other_imag = member[1]
        new_real = jnp.kron(real_part, other_real) - jnp.kron(imag_part, other_imag)
        new_imag = jnp.kron(real_part, other_imag) + jnp.kron(imag_part, other_real)
        real_part, imag_part = (new_real, new_imag)
    return (real_part, imag_part)


def rotate(flat, wide_count, narrow_count):
    devices = wide_count * narrow_count
    amplitudes = flat.shape[1]
    rest = amplitudes // devices
    blocks = flat.reshape(2, rest, devices)
    turned = jnp.swapaxes(blocks, 1, 2)
    moved = lax.all_to_all(turned, ("wide", "narrow"), split_axis=1, concat_axis=1, tiled=True)
    return moved.reshape(2, amplitudes)


def apply_layer(flat, layer_gates):
    amplitudes = flat.shape[1]
    pairs = layer_gates.shape[0]
    upper = amplitudes // 256
    low_real, low_imag = kron_chain([layer_gates[index] for index in range(3, -1, -1)])
    high_real, high_imag = kron_chain([layer_gates[index] for index in range(pairs - 1, 3, -1)])
    blocks = flat.reshape(2, upper, 256)
    real_rows = blocks[0]
    imag_rows = blocks[1]
    highest = lax.Precision.HIGHEST
    next_real = jnp.dot(real_rows, low_real.T, precision=highest) - jnp.dot(
        imag_rows, low_imag.T, precision=highest
    )
    next_imag = jnp.dot(real_rows, low_imag.T, precision=highest) + jnp.dot(
        imag_rows, low_real.T, precision=highest
    )
    final_real = jnp.dot(high_real, next_real, precision=highest) - jnp.dot(
        high_imag, next_imag, precision=highest
    )
    final_imag = jnp.dot(high_imag, next_real, precision=highest) + jnp.dot(
        high_real, next_imag, precision=highest
    )
    return jnp.stack([final_real, final_imag]).reshape(2, amplitudes)


MESH = pl.DeviceIdType.MESH
LANES = 128


def complex_mul(left, right):
    return (
        left[0] * right[0] - left[1] * right[1],
        left[0] * right[1] + left[1] * right[0],
    )


def small_matmul(left, right):
    total = None
    for index in range(right[0].shape[0]):
        column = tuple(part[:, index : index + 1] for part in left)
        row = tuple(part[index : index + 1, :] for part in right)
        term = complex_mul(column, row)
        total = term if total is None else tuple(a + b for a, b in zip(total, term))
    return total


def merged_gate(gate_ref, layers, pairs, shift, total_pairs, which):
    product = None
    for layer in range(layers):
        index = (which - layer * shift) % total_pairs
        if index < pairs:
            at = (layer * pairs + index) * 2
            gate = (gate_ref[at], gate_ref[at + 1])
            product = gate if product is None else small_matmul(gate, product)
    return product


def kron_all(members):
    radix = members[0][0].shape[0]
    size = radix ** len(members)
    lane = lax.broadcasted_iota(jnp.int32, (1, size), 1)
    rows = None
    for place, member in enumerate(reversed(members)):
        field = (lane // radix**place) % radix
        wide = []
        for part in member:
            spread = jnp.broadcast_to(part[:, radix - 1 : radix], (radix, size))
            for index in range(radix - 1):
                spread = jnp.where(field == index, part[:, index : index + 1], spread)
            wide.append(spread)
        if rows is None:
            rows = tuple(wide)
            continue
        pieces = [
            complex_mul(tuple(part[index : index + 1, :] for part in wide), rows)
            for index in range(radix)
        ]
        rows = tuple(jnp.concatenate([piece[c] for piece in pieces], axis=0) for c in range(2))
    return rows


def split(value):
    high = value.astype(jnp.bfloat16)
    return high, (value - high.astype(jnp.float32)).astype(jnp.bfloat16)


def dot_t(left, right):
    def one(a, b):
        return lax.dot_general(a, b, (((1,), (1,)), ((), ())), preferred_element_type=jnp.float32)

    return one(left[0], right[0]) + (one(left[0], right[1]) + one(left[1], right[0]))


def window_kernel(plan, x_hbm, g_hbm, out_hbm, marg_hbm, x, g, send, recv, fin, prob, part, marg,
                  local_sem, send_sem, recv_sem, psend_sem, precv_sem):
    layers, pairs, shift, total_pairs, start, radix = plan
    w = lax.axis_index("wide")
    n = lax.axis_index("narrow")
    offsets = [(dw, dn) for dw in range(radix) for dn in range(radix) if dw or dn]

    def partner(dw, dn):
        return lax.rem(w + dw, radix), lax.rem(n + dn, radix)

    barrier = pltpu.get_barrier_semaphore()
    for dw, dn in offsets:
        pw, pn = partner(dw, dn)
        pl.semaphore_signal(barrier, inc=1, device_id={"wide": pw, "narrow": pn}, device_id_type=MESH)
    copy_g = pltpu.make_async_copy(g_hbm, g, local_sem.at[0])
    copy_x = pltpu.make_async_copy(x_hbm, x, local_sem.at[1])
    copy_g.start()
    copy_x.start()
    copy_g.wait()

    gate_of = functools.partial(merged_gate, g, layers, pairs, shift, total_pairs)
    low_gate = gate_of(start)
    high_gate = gate_of(start + 1)

    half = LANES // 2
    rows_hi = send.shape[1]
    lane = lax.broadcasted_iota(jnp.int32, (rows_hi, LANES), 1)
    first = lane < half
    shape = (rows_hi, LANES)

    def entry(gate, row, column):
        return tuple(
            jnp.broadcast_to(part_[row : row + 1, column : column + 1], shape) for part_ in gate
        )

    def both(gate, one, other):
        return tuple(jnp.where(first, a, b) for a, b in zip(entry(gate, *one), entry(gate, *other)))

    def add(total, term):
        return term if total is None else (total[0] + term[0], total[1] + term[1])

    copy_x.wait()
    same = [[both(low_gate, (2 * o, 2 * i), (2 * o + 1, 2 * i + 1)) for i in range(2)] for o in range(2)]
    cross = [[both(low_gate, (2 * o, 2 * i + 1), (2 * o + 1, 2 * i)) for i in range(2)] for o in range(2)]
    stage = []
    stride = 4 * radix
    for high in range(radix):
        held = []
        for i in range(2):
            held.append(tuple(x[pl.ds(high * 4 + i * 2 + c, rows_hi, stride=stride), :] for c in range(2)))
        turned = [tuple(pltpu.roll(v, half, 1) for v in pair) for pair in held]
        result = []
        for o in range(2):
            total = None
            for i in range(2):
                total = add(total, complex_mul(same[o][i], held[i]))
                total = add(total, complex_mul(cross[o][i], turned[i]))
            result.append(total)
        stage.append(result)
    for out_high in range(radix):
        coefs = [entry(high_gate, out_high, high) for high in range(radix)]
        for o in range(2):
            total = None
            for high in range(radix):
                total = add(total, complex_mul(coefs[high], stage[high][o]))
            rolled = tuple(pltpu.roll(v, half, 1) for v in total)
            send[out_high * radix + 2 * o] = jnp.where(first, total[0], rolled[1])
            send[out_high * radix + 2 * o + 1] = jnp.where(first, rolled[0], total[1])

    pl.semaphore_wait(barrier, len(offsets))
    me = w * radix + n
    copies = []
    for at, (dw, dn) in enumerate(offsets):
        pw, pn = partner(dw, dn)
        copy = pltpu.make_async_remote_copy(
            src_ref=send.at[pw * radix + pn],
            dst_ref=recv.at[me],
            send_sem=send_sem.at[at],
            recv_sem=recv_sem.at[at],
            device_id={"wide": pw, "narrow": pn},
            device_id_type=MESH,
        )
        copy.start()
        copies.append(copy)
    recv[me] = send[me]

    low = kron_all([gate_of(which) for which in range(start - 1, -1, -1)])
    lane_form = split(
        jnp.concatenate(
            [
                jnp.concatenate([low[0], -low[1]], axis=1),
                jnp.concatenate([low[1], low[0]], axis=1),
            ],
            axis=0,
        )
    )
    row_real, row_imag = kron_all([gate_of(which) for which in range(total_pairs - 1, start + 1, -1)])
    row_real = split(row_real)
    row_imag = split(row_imag)

    for copy in copies:
        copy.wait_recv()
    count = radix * radix
    size = count * rows_hi
    turned = split(dot_t(lane_form, split(recv[...].reshape(size, LANES))))
    with_real = dot_t(turned, row_real)
    with_imag = dot_t(turned, row_imag)
    real = with_real[:half] - with_imag[half:]
    imag = with_real[half:] + with_imag[:half]
    density = real * real + imag * imag
    own_rows = half // radix
    for index in range(radix):
        prob[index] = density[index * own_rows : (index + 1) * own_rows]
    blocks = size // LANES
    for block in range(blocks):
        columns = slice(block * LANES, (block + 1) * LANES)
        fin[pl.ds(block * 2, half, stride=2 * blocks), :] = real[:, columns]
        fin[pl.ds(block * 2 + 1, half, stride=2 * blocks), :] = imag[:, columns]
    sums = []
    for dn in range(1, radix):
        pn = lax.rem(n + dn, radix)
        copy = pltpu.make_async_remote_copy(
            src_ref=prob.at[pn],
            dst_ref=part.at[dn - 1],
            send_sem=psend_sem.at[dn - 1],
            recv_sem=precv_sem.at[dn - 1],
            device_id={"wide": w, "narrow": pn},
            device_id_type=MESH,
        )
        copy.start()
        sums.append(copy)
    out_copy = pltpu.make_async_copy(fin, out_hbm, local_sem.at[0])
    out_copy.start()
    for copy in copies:
        copy.wait_send()
    total = prob[n]
    for index, copy in enumerate(sums):
        copy.wait_recv()
        total = total + part[index]
    for block in range(blocks):
        marg[pl.ds(block, own_rows, stride=blocks), :] = total[:, block * LANES : (block + 1) * LANES]
    marg_copy = pltpu.make_async_copy(marg, marg_hbm, local_sem.at[1])
    marg_copy.start()
    for copy in sums:
        copy.wait_send()
    out_copy.wait()
    marg_copy.wait()


def window_plan(wide_count, narrow_count, amplitudes, gates_shape):
    layers, pairs, radix = gates_shape[0], gates_shape[1], gates_shape[-1]
    high_bits = (wide_count * narrow_count).bit_length() - 1
    local_bits = amplitudes.bit_length() - 1
    total_bits = high_bits + local_bits
    if high_bits % 2 or local_bits % 2 or wide_count != radix or narrow_count != radix:
        return None
    if 2 * pairs != local_bits:
        return None
    offset = ((layers - 1) * high_bits) % total_bits
    start = offset // 2 - high_bits // 2
    if start < 1 or offset // 2 >= pairs or 2 * radix**start != LANES:
        return None
    rows_hi = radix ** (pairs - offset // 2)
    if rows_hi % 8:
        return None
    for which in range(total_bits // 2):
        if all((which - layer * (high_bits // 2)) % (total_bits // 2) >= pairs for layer in range(layers)):
            return None
    return (layers, pairs, high_bits // 2, total_bits // 2, start, radix), rows_hi


def merged_local(plan, rows_hi, state, gates):
    radix = plan[-1]
    amplitudes = state.shape[-1]
    rows = amplitudes // LANES
    count = radix * radix
    own = amplitudes // radix // LANES
    x = jnp.swapaxes(state.reshape(2, rows, LANES), 0, 1).reshape(2 * rows, LANES)
    g = gates.reshape(-1, radix, radix)
    f32 = jnp.float32
    wide_lanes = count * rows_hi
    chunk = (LANES // 2 // radix, wide_lanes)
    out, marg = pl.pallas_call(
        functools.partial(window_kernel, plan),
        out_shape=(
            jax.ShapeDtypeStruct((2 * rows, LANES), f32),
            jax.ShapeDtypeStruct((own, LANES), f32),
        ),
        in_specs=[pl.BlockSpec(memory_space=pl.ANY)] * 2,
        out_specs=[pl.BlockSpec(memory_space=pl.ANY)] * 2,
        scratch_shapes=[
            pltpu.VMEM(x.shape, f32),
            pltpu.VMEM(g.shape, f32),
            pltpu.VMEM((count, rows_hi, LANES), f32),
            pltpu.VMEM((count, rows_hi, LANES), f32),
            pltpu.VMEM((2 * rows, LANES), f32),
            pltpu.VMEM((radix,) + chunk, f32),
            pltpu.VMEM((radix - 1,) + chunk, f32),
            pltpu.VMEM((own, LANES), f32),
            pltpu.SemaphoreType.DMA((2,)),
            pltpu.SemaphoreType.DMA((count - 1,)),
            pltpu.SemaphoreType.DMA((count - 1,)),
            pltpu.SemaphoreType.DMA((radix - 1,)),
            pltpu.SemaphoreType.DMA((radix - 1,)),
        ],
        compiler_params=pltpu.CompilerParams(collective_id=0, has_side_effects=True),
        name="window",
    )(x, g)
    final = jnp.swapaxes(out.reshape(rows, 2, LANES), 0, 1).reshape(1, 1, 2, amplitudes)
    return final, marg.reshape(1, -1)


def local(state, gates):
    wide_count = lax.axis_size("wide")
    narrow_count = lax.axis_size("narrow")
    amplitudes = state.shape[-1]
    found = window_plan(wide_count, narrow_count, amplitudes, gates.shape)
    if found is not None:
        return merged_local(*found, state, gates)
    flat = state.reshape(2, amplitudes)
    for layer_index in range(gates.shape[0]):
        if layer_index > 0:
            flat = rotate(flat, wide_count, narrow_count)
        flat = apply_layer(flat, gates[layer_index])
    prob = flat[0] * flat[0] + flat[1] * flat[1]
    marginal = lax.psum_scatter(prob, "narrow", scatter_dimension=0, tiled=True)
    return (flat.reshape(1, 1, 2, amplitudes), marginal.reshape(1, -1))


def solution(mesh):
    in_specs = (P(("slices", "wide"), "narrow", None, None), P())
    out_specs = (P(("slices", "wide"), "narrow", None, None), P(("slices", "wide"), "narrow"))
    return jax.shard_map(local, mesh=mesh, in_specs=in_specs, out_specs=out_specs, check_vma=False)
```

```python
import functools

import jax
import jax.numpy as jnp
from jax import lax
from jax.experimental import pallas as pl
from jax.experimental.pallas import tpu as pltpu
from jax.sharding import PartitionSpec as P


def kron_chain(members):
    real_part = members[0][0]
    imag_part = members[0][1]
    for member in members[1:]:
        other_real = member[0]
        other_imag = member[1]
        new_real = jnp.kron(real_part, other_real) - jnp.kron(imag_part, other_imag)
        new_imag = jnp.kron(real_part, other_imag) + jnp.kron(imag_part, other_real)
        real_part, imag_part = (new_real, new_imag)
    return (real_part, imag_part)


def rotate(flat, wide_count, narrow_count):
    devices = wide_count * narrow_count
    amplitudes = flat.shape[1]
    rest = amplitudes // devices
    blocks = flat.reshape(2, rest, devices)
    turned = jnp.swapaxes(blocks, 1, 2)
    moved = lax.all_to_all(turned, ("wide", "narrow"), split_axis=1, concat_axis=1, tiled=True)
    return moved.reshape(2, amplitudes)


def apply_layer(flat, layer_gates):
    amplitudes = flat.shape[1]
    pairs = layer_gates.shape[0]
    upper = amplitudes // 256
    low_real, low_imag = kron_chain([layer_gates[index] for index in range(3, -1, -1)])
    high_real, high_imag = kron_chain([layer_gates[index] for index in range(pairs - 1, 3, -1)])
    blocks = flat.reshape(2, upper, 256)
    real_rows = blocks[0]
    imag_rows = blocks[1]
    highest = lax.Precision.HIGHEST
    next_real = jnp.dot(real_rows, low_real.T, precision=highest) - jnp.dot(
        imag_rows, low_imag.T, precision=highest
    )
    next_imag = jnp.dot(real_rows, low_imag.T, precision=highest) + jnp.dot(
        imag_rows, low_real.T, precision=highest
    )
    final_real = jnp.dot(high_real, next_real, precision=highest) - jnp.dot(
        high_imag, next_imag, precision=highest
    )
    final_imag = jnp.dot(high_imag, next_real, precision=highest) + jnp.dot(
        high_real, next_imag, precision=highest
    )
    return jnp.stack([final_real, final_imag]).reshape(2, amplitudes)


MESH = pl.DeviceIdType.MESH
LANES = 128


def complex_mul(left, right):
    return (
        left[0] * right[0] - left[1] * right[1],
        left[0] * right[1] + left[1] * right[0],
    )


def merged_gate(planes, layers, pairs, shift, total_pairs, which):
    product = None
    radix = planes[0][0].shape[0]
    for layer in range(layers):
        index = (which - layer * shift) % total_pairs
        if index >= pairs:
            continue
        plane = planes[index]
        if product is not None:
            total = None
            for row in range(radix):
                lane = row * layers + last
                column = tuple(part[:, lane : lane + 1] for part in product)
                term = complex_mul(column, tuple(part[row : row + 1, :] for part in plane))
                total = term if total is None else (total[0] + term[0], total[1] + term[1])
            plane = total
        product, last = plane, layer
    return product, last


def kron_all(members, layers):
    radix = members[0][0][0].shape[0]
    size = radix ** len(members)
    lane = lax.broadcasted_iota(jnp.int32, (1, size), 1)
    rows = None
    for place, (member, last) in enumerate(reversed(members)):
        field = (lane // radix**place) % radix
        wide = []
        for part in member:
            columns = [part[:, index * layers + last : index * layers + last + 1] for index in range(radix)]
            spread = jnp.broadcast_to(columns[-1], (radix, size))
            for index in range(radix - 1):
                spread = jnp.where(field == index, columns[index], spread)
            wide.append(spread)
        if rows is None:
            rows = tuple(wide)
            continue
        pieces = [
            complex_mul(tuple(part[index : index + 1, :] for part in wide), rows)
            for index in range(radix)
        ]
        rows = tuple(jnp.concatenate([piece[c] for piece in pieces], axis=0) for c in range(2))
    return rows


def split(value):
    high = value.astype(jnp.bfloat16)
    return high, (value - high.astype(jnp.float32)).astype(jnp.bfloat16)


def dot(left, right, contract):
    def one(a, b):
        return lax.dot_general(a, b, (((1,), (contract,)), ((), ())), preferred_element_type=jnp.float32)

    return one(left[0], right[0]) + (one(left[0], right[1]) + one(left[1], right[0]))


def window_kernel(plan, x_hbm, g_hbm, out_hbm, marg_hbm, x, g, send, recv, fin, prob, part, marg,
                  local_sem, send_sem, recv_sem, psend_sem, precv_sem):
    layers, pairs, shift, total_pairs, start, radix = plan
    w = lax.axis_index("wide")
    n = lax.axis_index("narrow")
    offsets = [(dw, dn) for dw in range(radix) for dn in range(radix) if dw or dn]

    def partner(dw, dn):
        return lax.rem(w + dw, radix), lax.rem(n + dn, radix)

    barrier = pltpu.get_barrier_semaphore()
    for dw, dn in offsets:
        pw, pn = partner(dw, dn)
        pl.semaphore_signal(barrier, inc=1, device_id={"wide": pw, "narrow": pn}, device_id_type=MESH)
    copy_g = pltpu.make_async_copy(g_hbm, g, local_sem.at[0])
    copy_x = pltpu.make_async_copy(x_hbm, x, local_sem.at[1])
    copy_g.start()
    copy_x.start()
    copy_g.wait()

    planes = []
    for index in range(pairs):
        plane = []
        for c in range(2):
            total = None
            for row in range(radix):
                tile = g[(index * 2 + c) * radix + row]
                tile = jnp.concatenate([tile, jnp.zeros((radix, LANES - layers), jnp.float32)], axis=1)
                tile = pltpu.roll(tile, row * layers, 1) if row else tile
                total = tile if total is None else total + tile
            plane.append(total)
        planes.append(tuple(plane))
    gate_of = functools.partial(merged_gate, planes, layers, pairs, shift, total_pairs)
    low_gate = gate_of(start)
    high_gate = gate_of(start + 1)

    half = LANES // 2
    rows_hi = send.shape[1]
    lane = lax.broadcasted_iota(jnp.int32, (rows_hi, LANES), 1)
    first = lane < half
    shape = (rows_hi, LANES)

    def entry(gate, row, column):
        lane_at = row * layers + gate[1]
        return tuple(
            jnp.broadcast_to(item[column : column + 1, lane_at : lane_at + 1], shape) for item in gate[0]
        )

    def both(gate, one, other):
        return tuple(jnp.where(first, a, b) for a, b in zip(entry(gate, *one), entry(gate, *other)))

    def add(total, term):
        return term if total is None else (total[0] + term[0], total[1] + term[1])

    copy_x.wait()
    same = [[both(low_gate, (2 * o, 2 * i), (2 * o + 1, 2 * i + 1)) for i in range(2)] for o in range(2)]
    cross = [[both(low_gate, (2 * o, 2 * i + 1), (2 * o + 1, 2 * i)) for i in range(2)] for o in range(2)]
    stage = []
    stride = 4 * radix
    for high in range(radix):
        held = []
        for i in range(2):
            held.append(tuple(x[pl.ds(high * 4 + i * 2 + c, rows_hi, stride=stride), :] for c in range(2)))
        turned = [tuple(pltpu.roll(v, half, 1) for v in pair) for pair in held]
        result = []
        for o in range(2):
            total = None
            for i in range(2):
                total = add(total, complex_mul(same[o][i], held[i]))
                total = add(total, complex_mul(cross[o][i], turned[i]))
            result.append(total)
        stage.append(result)
    for out_high in range(radix):
        coefs = [entry(high_gate, out_high, high) for high in range(radix)]
        for o in range(2):
            total = None
            for high in range(radix):
                total = add(total, complex_mul(coefs[high], stage[high][o]))
            rolled = tuple(pltpu.roll(v, half, 1) for v in total)
            send[out_high * radix + 2 * o] = jnp.where(first, total[0], rolled[1])
            send[out_high * radix + 2 * o + 1] = jnp.where(first, rolled[0], total[1])

    pl.semaphore_wait(barrier, len(offsets))
    me = w * radix + n
    copies = []
    for at, (dw, dn) in enumerate(offsets):
        pw, pn = partner(dw, dn)
        copy = pltpu.make_async_remote_copy(
            src_ref=send.at[pw * radix + pn],
            dst_ref=recv.at[me],
            send_sem=send_sem.at[at],
            recv_sem=recv_sem.at[at],
            device_id={"wide": pw, "narrow": pn},
            device_id_type=MESH,
        )
        copy.start()
        copies.append(copy)
    recv[me] = send[me]

    low = kron_all([gate_of(which) for which in range(start - 1, -1, -1)], layers)
    lane_form = jnp.concatenate(
        [
            jnp.concatenate([low[0], low[1]], axis=1),
            jnp.concatenate([-low[1], low[0]], axis=1),
        ],
        axis=0,
    )
    lane_form = split(lane_form.T)
    row_members = [gate_of(which) for which in range(total_pairs - 1, start + 1, -1)]
    row_real, row_imag = (split(item) for item in kron_all(row_members, layers))

    for copy in copies:
        copy.wait_recv()
    count = radix * radix
    size = count * rows_hi
    turned = split(dot(lane_form, split(recv[...].reshape(size, LANES)), 1))
    with_real = dot(turned, row_real, 0)
    with_imag = dot(turned, row_imag, 0)
    real = with_real[:half] - with_imag[half:]
    imag = with_real[half:] + with_imag[:half]
    density = real * real + imag * imag
    own_rows = half // radix
    for index in range(radix):
        prob[index] = density[index * own_rows : (index + 1) * own_rows]
    blocks = size // LANES
    for block in range(blocks):
        columns = slice(block * LANES, (block + 1) * LANES)
        fin[pl.ds(block * 2, half, stride=2 * blocks), :] = real[:, columns]
        fin[pl.ds(block * 2 + 1, half, stride=2 * blocks), :] = imag[:, columns]
    sums = []
    for dn in range(1, radix):
        pn = lax.rem(n + dn, radix)
        copy = pltpu.make_async_remote_copy(
            src_ref=prob.at[pn],
            dst_ref=part.at[dn - 1],
            send_sem=psend_sem.at[dn - 1],
            recv_sem=precv_sem.at[dn - 1],
            device_id={"wide": w, "narrow": pn},
            device_id_type=MESH,
        )
        copy.start()
        sums.append(copy)
    out_copy = pltpu.make_async_copy(fin, out_hbm, local_sem.at[0])
    out_copy.start()
    for copy in copies:
        copy.wait_send()
    total = prob[n]
    for index, copy in enumerate(sums):
        copy.wait_recv()
        total = total + part[index]
    for block in range(blocks):
        marg[pl.ds(block, own_rows, stride=blocks), :] = total[:, block * LANES : (block + 1) * LANES]
    marg_copy = pltpu.make_async_copy(marg, marg_hbm, local_sem.at[1])
    marg_copy.start()
    for copy in sums:
        copy.wait_send()
    out_copy.wait()
    marg_copy.wait()


def window_plan(wide_count, narrow_count, amplitudes, gates_shape):
    layers, pairs, radix = gates_shape[0], gates_shape[1], gates_shape[-1]
    high_bits = (wide_count * narrow_count).bit_length() - 1
    local_bits = amplitudes.bit_length() - 1
    total_bits = high_bits + local_bits
    if high_bits % 2 or local_bits % 2 or wide_count != radix or narrow_count != radix:
        return None
    if 2 * pairs != local_bits:
        return None
    offset = ((layers - 1) * high_bits) % total_bits
    start = offset // 2 - high_bits // 2
    if layers * radix > LANES or start < 1 or offset // 2 >= pairs or 2 * radix**start != LANES:
        return None
    rows_hi = radix ** (pairs - offset // 2)
    if rows_hi % 8:
        return None
    for which in range(total_bits // 2):
        if all((which - layer * (high_bits // 2)) % (total_bits // 2) >= pairs for layer in range(layers)):
            return None
    return (layers, pairs, high_bits // 2, total_bits // 2, start, radix), rows_hi


def merged_local(plan, rows_hi, state, gates):
    radix = plan[-1]
    amplitudes = state.shape[-1]
    rows = amplitudes // LANES
    count = radix * radix
    own = amplitudes // radix // LANES
    x = jnp.swapaxes(state.reshape(2, rows, LANES), 0, 1).reshape(2 * rows, LANES)
    g = jnp.transpose(gates, (1, 2, 3, 4, 0)).reshape(-1, radix, gates.shape[0])
    f32 = jnp.float32
    wide_lanes = count * rows_hi
    chunk = (LANES // 2 // radix, wide_lanes)
    out, marg = pl.pallas_call(
        functools.partial(window_kernel, plan),
        out_shape=(
            jax.ShapeDtypeStruct((2 * rows, LANES), f32),
            jax.ShapeDtypeStruct((own, LANES), f32),
        ),
        in_specs=[pl.BlockSpec(memory_space=pltpu.HBM)] * 2,
        out_specs=[pl.BlockSpec(memory_space=pl.ANY)] * 2,
        scratch_shapes=[
            pltpu.VMEM(x.shape, f32),
            pltpu.VMEM(g.shape, f32),
            pltpu.VMEM((count, rows_hi, LANES), f32),
            pltpu.VMEM((count, rows_hi, LANES), f32),
            pltpu.VMEM((2 * rows, LANES), f32),
            pltpu.VMEM((radix,) + chunk, f32),
            pltpu.VMEM((radix - 1,) + chunk, f32),
            pltpu.VMEM((own, LANES), f32),
            pltpu.SemaphoreType.DMA((2,)),
            pltpu.SemaphoreType.DMA((count - 1,)),
            pltpu.SemaphoreType.DMA((count - 1,)),
            pltpu.SemaphoreType.DMA((radix - 1,)),
            pltpu.SemaphoreType.DMA((radix - 1,)),
        ],
        compiler_params=pltpu.CompilerParams(
            collective_id=0, has_side_effects=True, vmem_limit_bytes=8 * 2**20
        ),
        name="window",
    )(x, g)
    final = jnp.swapaxes(out.reshape(rows, 2, LANES), 0, 1).reshape(1, 1, 2, amplitudes)
    return final, marg.reshape(1, -1)


def local(state, gates):
    wide_count = lax.axis_size("wide")
    narrow_count = lax.axis_size("narrow")
    amplitudes = state.shape[-1]
    found = window_plan(wide_count, narrow_count, amplitudes, gates.shape)
    if found is not None:
        return merged_local(*found, state, gates)
    flat = state.reshape(2, amplitudes)
    for layer_index in range(gates.shape[0]):
        if layer_index > 0:
            flat = rotate(flat, wide_count, narrow_count)
        flat = apply_layer(flat, gates[layer_index])
    prob = flat[0] * flat[0] + flat[1] * flat[1]
    marginal = lax.psum_scatter(prob, "narrow", scatter_dimension=0, tiled=True)
    return (flat.reshape(1, 1, 2, amplitudes), marginal.reshape(1, -1))


def solution(mesh):
    in_specs = (P(("slices", "wide"), "narrow", None, None), P())
    out_specs = (P(("slices", "wide"), "narrow", None, None), P(("slices", "wide"), "narrow"))
    return jax.shard_map(local, mesh=mesh, in_specs=in_specs, out_specs=out_specs, check_vma=False)
```

```python
import functools

import jax
import jax.numpy as jnp
from jax import lax
from jax.experimental import pallas as pl
from jax.experimental.pallas import tpu as pltpu
from jax.sharding import PartitionSpec as P


def kron_chain(members):
    real_part = members[0][0]
    imag_part = members[0][1]
    for member in members[1:]:
        other_real = member[0]
        other_imag = member[1]
        new_real = jnp.kron(real_part, other_real) - jnp.kron(imag_part, other_imag)
        new_imag = jnp.kron(real_part, other_imag) + jnp.kron(imag_part, other_real)
        real_part, imag_part = (new_real, new_imag)
    return (real_part, imag_part)


def rotate(flat, wide_count, narrow_count):
    devices = wide_count * narrow_count
    amplitudes = flat.shape[1]
    rest = amplitudes // devices
    blocks = flat.reshape(2, rest, devices)
    turned = jnp.swapaxes(blocks, 1, 2)
    moved = lax.all_to_all(turned, ("wide", "narrow"), split_axis=1, concat_axis=1, tiled=True)
    return moved.reshape(2, amplitudes)


def apply_layer(flat, layer_gates):
    amplitudes = flat.shape[1]
    pairs = layer_gates.shape[0]
    upper = amplitudes // 256
    low_real, low_imag = kron_chain([layer_gates[index] for index in range(3, -1, -1)])
    high_real, high_imag = kron_chain([layer_gates[index] for index in range(pairs - 1, 3, -1)])
    blocks = flat.reshape(2, upper, 256)
    real_rows = blocks[0]
    imag_rows = blocks[1]
    highest = lax.Precision.HIGHEST
    next_real = jnp.dot(real_rows, low_real.T, precision=highest) - jnp.dot(
        imag_rows, low_imag.T, precision=highest
    )
    next_imag = jnp.dot(real_rows, low_imag.T, precision=highest) + jnp.dot(
        imag_rows, low_real.T, precision=highest
    )
    final_real = jnp.dot(high_real, next_real, precision=highest) - jnp.dot(
        high_imag, next_imag, precision=highest
    )
    final_imag = jnp.dot(high_imag, next_real, precision=highest) + jnp.dot(
        high_real, next_imag, precision=highest
    )
    return jnp.stack([final_real, final_imag]).reshape(2, amplitudes)


MESH = pl.DeviceIdType.MESH
LANES = 128


def complex_mul(left, right):
    return (
        left[0] * right[0] - left[1] * right[1],
        left[0] * right[1] + left[1] * right[0],
    )


def merged_gate(planes, layers, pairs, shift, total_pairs, which):
    product = None
    radix = planes[0][0].shape[0]
    for layer in range(layers):
        index = (which - layer * shift) % total_pairs
        if index >= pairs:
            continue
        plane = planes[index]
        if product is not None:
            total = None
            for row in range(radix):
                lane = row * layers + last
                column = tuple(part[:, lane : lane + 1] for part in product)
                term = complex_mul(column, tuple(part[row : row + 1, :] for part in plane))
                total = term if total is None else (total[0] + term[0], total[1] + term[1])
            plane = total
        product, last = plane, layer
    return product, last


def kron_all(members, layers):
    radix = members[0][0][0].shape[0]
    size = radix ** len(members)
    lane = lax.broadcasted_iota(jnp.int32, (1, size), 1)
    rows = None
    for place, (member, last) in enumerate(reversed(members)):
        field = (lane // radix**place) % radix
        wide = []
        for part in member:
            columns = [part[:, index * layers + last : index * layers + last + 1] for index in range(radix)]
            spread = jnp.broadcast_to(columns[-1], (radix, size))
            for index in range(radix - 1):
                spread = jnp.where(field == index, columns[index], spread)
            wide.append(spread)
        if rows is None:
            rows = tuple(wide)
            continue
        pieces = [
            complex_mul(tuple(part[index : index + 1, :] for part in wide), rows)
            for index in range(radix)
        ]
        rows = tuple(jnp.concatenate([piece[c] for piece in pieces], axis=0) for c in range(2))
    return rows


def split(value):
    high = value.astype(jnp.bfloat16)
    return high, (value - high.astype(jnp.float32)).astype(jnp.bfloat16)


def dot(left, right, contract):
    def one(a, b):
        return lax.dot_general(a, b, (((1,), (contract,)), ((), ())), preferred_element_type=jnp.float32)

    return one(left[0], right[0]) + (one(left[0], right[1]) + one(left[1], right[0]))


def exchange_kernel(plan, x_hbm, g_hbm, recv, lane_hi, lane_lo, row_hi, row_lo, x, g, send,
                    local_sem, send_sem, recv_sem):
    layers, pairs, shift, total_pairs, start, radix = plan
    w = lax.axis_index("wide")
    n = lax.axis_index("narrow")
    offsets = [(dw, dn) for dw in range(radix) for dn in range(radix) if dw or dn]

    def partner(dw, dn):
        return lax.rem(w + dw, radix), lax.rem(n + dn, radix)

    barrier = pltpu.get_barrier_semaphore()
    for dw, dn in offsets:
        pw, pn = partner(dw, dn)
        pl.semaphore_signal(barrier, inc=1, device_id={"wide": pw, "narrow": pn}, device_id_type=MESH)
    copy_g = pltpu.make_async_copy(g_hbm, g, local_sem.at[0])
    copy_x = pltpu.make_async_copy(x_hbm, x, local_sem.at[1])
    copy_g.start()
    copy_x.start()
    copy_g.wait()

    planes = []
    for index in range(pairs):
        plane = []
        for c in range(2):
            total = None
            for row in range(radix):
                tile = g[(index * 2 + c) * radix + row]
                tile = jnp.concatenate([tile, jnp.zeros((radix, LANES - layers), jnp.float32)], axis=1)
                tile = pltpu.roll(tile, row * layers, 1) if row else tile
                total = tile if total is None else total + tile
            plane.append(total)
        planes.append(tuple(plane))
    gate_of = functools.partial(merged_gate, planes, layers, pairs, shift, total_pairs)
    split_gate = gate_of(start - 1)
    low_gate = gate_of(start)
    high_gate = gate_of(start + 1)

    half = LANES // 2
    group = half // radix
    rows_hi = send.shape[1] // 2
    shape = (rows_hi, LANES)
    lane = lax.broadcasted_iota(jnp.int32, shape, 1)
    first = lane < half
    field = (lane // group) % radix

    def entry(gate, row, column):
        lane_at = row * layers + gate[1]
        return tuple(
            jnp.broadcast_to(item[column : column + 1, lane_at : lane_at + 1], shape) for item in gate[0]
        )

    def both(gate, one, other):
        return tuple(jnp.where(first, a, b) for a, b in zip(entry(gate, *one), entry(gate, *other)))

    def add(total, term):
        return term if total is None else (total[0] + term[0], total[1] + term[1])

    def roll(value, amount):
        amount %= LANES
        return pltpu.roll(value, amount, 1) if amount else value

    steps = {}
    for row in range(radix):
        for column in range(radix):
            item = tuple(jnp.where(field == row, part, 0.0) for part in entry(split_gate, row, column))
            steps[column - row] = add(steps.get(column - row), item)

    copy_x.wait()
    same = [[both(low_gate, (2 * o, 2 * i), (2 * o + 1, 2 * i + 1)) for i in range(2)] for o in range(2)]
    cross = [[both(low_gate, (2 * o, 2 * i + 1), (2 * o + 1, 2 * i)) for i in range(2)] for o in range(2)]
    stage = []
    stride = 4 * radix
    for high in range(radix):
        held = []
        for i in range(2):
            held.append(tuple(x[pl.ds(high * 4 + i * 2 + c, rows_hi, stride=stride), :] for c in range(2)))
        turned = [tuple(roll(v, half) for v in pair) for pair in held]
        result = []
        for o in range(2):
            total = None
            for i in range(2):
                total = add(total, complex_mul(same[o][i], held[i]))
                total = add(total, complex_mul(cross[o][i], turned[i]))
            result.append(total)
        stage.append(result)
    for out_high in range(radix):
        coefs = [entry(high_gate, out_high, high) for high in range(radix)]
        ready = []
        for o in range(2):
            total = None
            for high in range(radix):
                total = add(total, complex_mul(coefs[high], stage[high][o]))
            mixed = None
            for step, coef in steps.items():
                mixed = add(mixed, complex_mul(coef, tuple(roll(v, -group * step) for v in total)))
            ready.append(mixed)
            rolled = tuple(roll(v, half) for v in mixed)
            at = out_high * radix + 2 * o
            send[at, :rows_hi] = jnp.where(first, mixed[0], rolled[1])
            send[at + 1, :rows_hi] = jnp.where(first, rolled[0], mixed[1])
        for take in range(radix):
            block = None
            for o in range(2):
                for c in range(2):
                    piece = roll(ready[o][c], (2 * o + c - take) * group)
                    block = piece if block is None else jnp.where(field == 2 * o + c, piece, block)
            send[out_high * radix + take, rows_hi:] = block

    pl.semaphore_wait(barrier, len(offsets))
    me = w * radix + n
    copies = []
    for at, (dw, dn) in enumerate(offsets):
        pw, pn = partner(dw, dn)
        copy = pltpu.make_async_remote_copy(
            src_ref=send.at[pw * radix + pn],
            dst_ref=recv.at[me],
            send_sem=send_sem.at[at],
            recv_sem=recv_sem.at[at],
            device_id={"wide": pw, "narrow": pn},
            device_id_type=MESH,
        )
        copy.start()
        copies.append(copy)
    recv[me] = send[me]

    low = kron_all([gate_of(which) for which in range(start - 2, -1, -1)], layers)
    block = jnp.concatenate(
        [jnp.concatenate([low[0], low[1]], axis=1), jnp.concatenate([-low[1], low[0]], axis=1)], axis=0
    )
    block = jnp.concatenate([jnp.concatenate([block] * radix, axis=0)] * radix, axis=1)
    down = lax.broadcasted_iota(jnp.int32, (LANES, LANES), 0)
    across = lax.broadcasted_iota(jnp.int32, (LANES, LANES), 1)
    grouped = jnp.where(down // (2 * group) == across // (2 * group), block, 0.0).T
    parts = [jnp.concatenate([jnp.concatenate([item] * radix, axis=0)] * radix, axis=1) for item in low]
    keep = (down[:half, :half] // group) == (across[:half, :half] // group)
    parts = [jnp.where(keep, item, 0.0) for item in parts]
    plain = jnp.concatenate(
        [jnp.concatenate([parts[0], parts[1]], axis=1), jnp.concatenate([-parts[1], parts[0]], axis=1)],
        axis=0,
    ).T
    for index, item in enumerate((plain, grouped)):
        lane_hi[index], lane_lo[index] = split(item)
    row_members = [gate_of(which) for which in range(total_pairs - 1, start + 1, -1)]
    for index, item in enumerate(kron_all(row_members, layers)):
        row_hi[index], row_lo[index] = split(item)

    for copy in copies:
        copy.wait()


def finish_kernel(radix, recv, lane_hi, lane_lo, row_hi, row_lo, out_hbm, marg_hbm, fin, marg, sems):
    rows_hi = recv.shape[1] // 2
    size = recv.shape[0] * rows_hi
    half = LANES // 2
    group = half // radix
    blocks = size // LANES
    rows = (row_hi[0], row_lo[0]), (row_hi[1], row_lo[1])

    def apply(which):
        held = split(recv[:, which * rows_hi : (which + 1) * rows_hi].reshape(size, LANES))
        turned = split(dot((lane_hi[which], lane_lo[which]), held, 1))
        return dot(turned, rows[0], 0), dot(turned, rows[1], 0)

    with_real, with_imag = apply(0)
    real = with_real[:half] - with_imag[half:]
    imag = with_real[half:] + with_imag[:half]
    for block in range(blocks):
        columns = slice(block * LANES, (block + 1) * LANES)
        fin[pl.ds(block * 2, half, stride=2 * blocks), :] = real[:, columns]
        fin[pl.ds(block * 2 + 1, half, stride=2 * blocks), :] = imag[:, columns]
    out_copy = pltpu.make_async_copy(fin, out_hbm, sems.at[0])
    out_copy.start()
    with_real, with_imag = apply(1)
    total = None
    for index in range(radix):
        at = 2 * group * index
        real = with_real[at : at + group] - with_imag[at + group : at + 2 * group]
        imag = with_real[at + group : at + 2 * group] + with_imag[at : at + group]
        term = real * real + imag * imag
        total = term if total is None else total + term
    for block in range(blocks):
        marg[pl.ds(block, group, stride=blocks), :] = total[:, block * LANES : (block + 1) * LANES]
    marg_copy = pltpu.make_async_copy(marg, marg_hbm, sems.at[1])
    marg_copy.start()
    out_copy.wait()
    marg_copy.wait()


def window_plan(wide_count, narrow_count, amplitudes, gates_shape):
    layers, pairs, radix = gates_shape[0], gates_shape[1], gates_shape[-1]
    high_bits = (wide_count * narrow_count).bit_length() - 1
    local_bits = amplitudes.bit_length() - 1
    total_bits = high_bits + local_bits
    if high_bits % 2 or local_bits % 2 or wide_count != radix or narrow_count != radix:
        return None
    if 2 * pairs != local_bits:
        return None
    offset = ((layers - 1) * high_bits) % total_bits
    start = offset // 2 - high_bits // 2
    if layers * radix > LANES or start < 2 or offset // 2 >= pairs or 2 * radix**start != LANES:
        return None
    rows_hi = radix ** (pairs - offset // 2)
    if rows_hi % 8:
        return None
    for which in range(total_bits // 2):
        if all((which - layer * (high_bits // 2)) % (total_bits // 2) >= pairs for layer in range(layers)):
            return None
    return (layers, pairs, high_bits // 2, total_bits // 2, start, radix), rows_hi


def merged_local(plan, rows_hi, state, gates):
    radix = plan[-1]
    amplitudes = state.shape[-1]
    rows = amplitudes // LANES
    count = radix * radix
    own = amplitudes // radix // LANES
    x = jnp.swapaxes(state.reshape(2, rows, LANES), 0, 1).reshape(2 * rows, LANES)
    g = jnp.transpose(gates, (1, 2, 3, 4, 0)).reshape(-1, radix, gates.shape[0])
    f32, bf16 = jnp.float32, jnp.bfloat16
    size = count * rows_hi
    shared = (
        pltpu.VMEM((count, 2 * rows_hi, LANES), f32),
        pltpu.VMEM((2, LANES, LANES), bf16),
        pltpu.VMEM((2, LANES, LANES), bf16),
        pltpu.VMEM((2, size, size), bf16),
        pltpu.VMEM((2, size, size), bf16),
    )
    held = pl.pallas_call(
        functools.partial(exchange_kernel, plan),
        out_shape=shared,
        in_specs=[pl.BlockSpec(memory_space=pltpu.HBM)] * 2,
        out_specs=[pl.BlockSpec(memory_space=pltpu.VMEM)] * len(shared),
        scratch_shapes=[
            pltpu.VMEM(x.shape, f32),
            pltpu.VMEM(g.shape, f32),
            pltpu.VMEM((count, 2 * rows_hi, LANES), f32),
            pltpu.SemaphoreType.DMA((2,)),
            pltpu.SemaphoreType.DMA((count - 1,)),
            pltpu.SemaphoreType.DMA((count - 1,)),
        ],
        compiler_params=pltpu.CompilerParams(
            collective_id=0, has_side_effects=True, vmem_limit_bytes=8 * 2**20
        ),
        name="exchange",
    )(
        pltpu.with_memory_space_constraint(x, pltpu.HBM),
        pltpu.with_memory_space_constraint(g, pltpu.HBM),
    )
    out, marg = pl.pallas_call(
        functools.partial(finish_kernel, radix),
        out_shape=(pltpu.HBM((2 * rows, LANES), f32), pltpu.HBM((own, LANES), f32)),
        in_specs=[pl.BlockSpec(memory_space=pltpu.VMEM)] * len(shared),
        out_specs=[pl.BlockSpec(memory_space=pltpu.HBM)] * 2,
        scratch_shapes=[
            pltpu.VMEM((2 * rows, LANES), f32),
            pltpu.VMEM((own, LANES), f32),
            pltpu.SemaphoreType.DMA((2,)),
        ],
        compiler_params=pltpu.CompilerParams(vmem_limit_bytes=8 * 2**20),
        name="finish",
    )(*held)
    final = jnp.swapaxes(out.reshape(rows, 2, LANES), 0, 1).reshape(1, 1, 2, amplitudes)
    return final, marg.reshape(1, -1)


def local(state, gates):
    wide_count = lax.axis_size("wide")
    narrow_count = lax.axis_size("narrow")
    amplitudes = state.shape[-1]
    found = window_plan(wide_count, narrow_count, amplitudes, gates.shape)
    if found is not None:
        return merged_local(*found, state, gates)
    flat = state.reshape(2, amplitudes)
    for layer_index in range(gates.shape[0]):
        if layer_index > 0:
            flat = rotate(flat, wide_count, narrow_count)
        flat = apply_layer(flat, gates[layer_index])
    prob = flat[0] * flat[0] + flat[1] * flat[1]
    marginal = lax.psum_scatter(prob, "narrow", scatter_dimension=0, tiled=True)
    return (flat.reshape(1, 1, 2, amplitudes), marginal.reshape(1, -1))


def solution(mesh):
    in_specs = (P(("slices", "wide"), "narrow", None, None), P())
    out_specs = (P(("slices", "wide"), "narrow", None, None), P(("slices", "wide"), "narrow"))
    return jax.shard_map(local, mesh=mesh, in_specs=in_specs, out_specs=out_specs, check_vma=False)
```

```python
import functools

import jax
import jax.numpy as jnp
from jax import lax
from jax.experimental import pallas as pl
from jax.experimental.pallas import tpu as pltpu
from jax.sharding import PartitionSpec as P


def kron_chain(members):
    real_part = members[0][0]
    imag_part = members[0][1]
    for member in members[1:]:
        other_real = member[0]
        other_imag = member[1]
        new_real = jnp.kron(real_part, other_real) - jnp.kron(imag_part, other_imag)
        new_imag = jnp.kron(real_part, other_imag) + jnp.kron(imag_part, other_real)
        real_part, imag_part = (new_real, new_imag)
    return (real_part, imag_part)


def rotate(flat, wide_count, narrow_count):
    devices = wide_count * narrow_count
    amplitudes = flat.shape[1]
    rest = amplitudes // devices
    blocks = flat.reshape(2, rest, devices)
    turned = jnp.swapaxes(blocks, 1, 2)
    moved = lax.all_to_all(turned, ("wide", "narrow"), split_axis=1, concat_axis=1, tiled=True)
    return moved.reshape(2, amplitudes)


def apply_layer(flat, layer_gates):
    amplitudes = flat.shape[1]
    pairs = layer_gates.shape[0]
    upper = amplitudes // 256
    low_real, low_imag = kron_chain([layer_gates[index] for index in range(3, -1, -1)])
    high_real, high_imag = kron_chain([layer_gates[index] for index in range(pairs - 1, 3, -1)])
    blocks = flat.reshape(2, upper, 256)
    real_rows = blocks[0]
    imag_rows = blocks[1]
    highest = lax.Precision.HIGHEST
    next_real = jnp.dot(real_rows, low_real.T, precision=highest) - jnp.dot(
        imag_rows, low_imag.T, precision=highest
    )
    next_imag = jnp.dot(real_rows, low_imag.T, precision=highest) + jnp.dot(
        imag_rows, low_real.T, precision=highest
    )
    final_real = jnp.dot(high_real, next_real, precision=highest) - jnp.dot(
        high_imag, next_imag, precision=highest
    )
    final_imag = jnp.dot(high_imag, next_real, precision=highest) + jnp.dot(
        high_real, next_imag, precision=highest
    )
    return jnp.stack([final_real, final_imag]).reshape(2, amplitudes)


MESH = pl.DeviceIdType.MESH
LANES = 128


def complex_mul(left, right):
    return (
        left[0] * right[0] - left[1] * right[1],
        left[0] * right[1] + left[1] * right[0],
    )


def merged_gates(planes, plan, which):
    layers, pairs, shift, total_pairs, _, radix = plan
    lane = lax.broadcasted_iota(jnp.int32, planes[0][0].shape, 1)
    down = lax.broadcasted_iota(jnp.int32, planes[0][0].shape, 0)
    unit = jnp.where(lane // layers == down, 1.0, 0.0)
    unit = (unit, jnp.zeros_like(unit))
    items = []
    for layer in range(layers):
        places = [(pair - layer * shift) % total_pairs for pair in which]
        chosen = [planes[place] if place < pairs else unit for place in places]
        items.append((tuple(jnp.stack([gate[c] for gate in chosen]) for c in range(2)), layer))
    while len(items) > 1:
        joined = []
        for at in range(0, len(items) - 1, 2):
            (early, last), (late, newest) = items[at], items[at + 1]
            total = None
            for row in range(radix):
                lane_at = row * layers + last
                term = complex_mul(
                    tuple(part[:, :, lane_at : lane_at + 1] for part in early),
                    tuple(part[:, row : row + 1, :] for part in late),
                )
                total = term if total is None else (total[0] + term[0], total[1] + term[1])
            joined.append((total, newest))
        if len(items) % 2:
            joined.append(items[-1])
        items = joined
    parts, last = items[0]
    return [(tuple(part[index] for part in parts), last) for index in range(len(which))]


def kron_all(members, layers):
    radix = members[0][0][0].shape[0]
    size = radix ** len(members)
    lane = lax.broadcasted_iota(jnp.int32, (1, size), 1)
    rows = None
    for place, (member, last) in enumerate(reversed(members)):
        field = (lane // radix**place) % radix
        wide = []
        for part in member:
            columns = [part[:, index * layers + last : index * layers + last + 1] for index in range(radix)]
            spread = jnp.broadcast_to(columns[-1], (radix, size))
            for index in range(radix - 1):
                spread = jnp.where(field == index, columns[index], spread)
            wide.append(spread)
        if rows is None:
            rows = tuple(wide)
            continue
        pieces = [
            complex_mul(tuple(part[index : index + 1, :] for part in wide), rows)
            for index in range(radix)
        ]
        rows = tuple(jnp.concatenate([piece[c] for piece in pieces], axis=0) for c in range(2))
    return rows


def split(value):
    high = value.astype(jnp.bfloat16)
    return high, (value - high.astype(jnp.float32)).astype(jnp.bfloat16)


def dot(left, right, contract):
    def one(a, b):
        return lax.dot_general(a, b, (((1,), (contract,)), ((), ())), preferred_element_type=jnp.float32)

    return one(left[0], right[0]) + (one(left[0], right[1]) + one(left[1], right[0]))


def exchange_kernel(plan, x_hbm, g_hbm, recv, lane_hi, lane_lo, row_hi, row_lo, x, g, send,
                    local_sem, send_sem, recv_sem):
    layers, pairs, shift, total_pairs, start, radix = plan
    w = lax.axis_index("wide")
    n = lax.axis_index("narrow")
    offsets = [(dw, dn) for dw in range(radix) for dn in range(radix) if dw or dn]

    def partner(dw, dn):
        return lax.rem(w + dw, radix), lax.rem(n + dn, radix)

    barrier = pltpu.get_barrier_semaphore()
    for dw, dn in offsets:
        pw, pn = partner(dw, dn)
        pl.semaphore_signal(barrier, inc=1, device_id={"wide": pw, "narrow": pn}, device_id_type=MESH)
    copy_g = pltpu.make_async_copy(g_hbm, g, local_sem.at[0])
    copy_x = pltpu.make_async_copy(x_hbm, x, local_sem.at[1])
    copy_g.start()
    copy_x.start()
    copy_g.wait()

    planes = []
    for index in range(pairs):
        plane = []
        for c in range(2):
            total = None
            for row in range(radix):
                tile = g[(index * 2 + c) * radix + row]
                tile = jnp.concatenate([tile, jnp.zeros((radix, LANES - layers), jnp.float32)], axis=1)
                tile = pltpu.roll(tile, row * layers, 1) if row else tile
                total = tile if total is None else total + tile
            plane.append(total)
        planes.append(tuple(plane))
    split_gate, low_gate, high_gate = merged_gates(planes, plan, range(start - 1, start + 2))

    half = LANES // 2
    group = half // radix
    rows_hi = send.shape[1] // 2
    shape = (rows_hi, LANES)
    lane = lax.broadcasted_iota(jnp.int32, shape, 1)
    first = lane < half
    field = (lane // group) % radix

    def entry(gate, row, column):
        lane_at = row * layers + gate[1]
        return tuple(
            jnp.broadcast_to(item[column : column + 1, lane_at : lane_at + 1], shape) for item in gate[0]
        )

    def both(gate, one, other):
        return tuple(jnp.where(first, a, b) for a, b in zip(entry(gate, *one), entry(gate, *other)))

    def add(total, term):
        return term if total is None else (total[0] + term[0], total[1] + term[1])

    def roll(value, amount):
        amount %= LANES
        return pltpu.roll(value, amount, 1) if amount else value

    steps = {}
    for row in range(radix):
        for column in range(radix):
            item = tuple(jnp.where(field == row, part, 0.0) for part in entry(split_gate, row, column))
            steps[column - row] = add(steps.get(column - row), item)

    copy_x.wait()
    same = [[both(low_gate, (2 * o, 2 * i), (2 * o + 1, 2 * i + 1)) for i in range(2)] for o in range(2)]
    cross = [[both(low_gate, (2 * o, 2 * i + 1), (2 * o + 1, 2 * i)) for i in range(2)] for o in range(2)]
    stage = []
    stride = 4 * radix
    for high in range(radix):
        held = []
        for i in range(2):
            held.append(tuple(x[pl.ds(high * 4 + i * 2 + c, rows_hi, stride=stride), :] for c in range(2)))
        turned = [tuple(roll(v, half) for v in pair) for pair in held]
        result = []
        for o in range(2):
            total = None
            for i in range(2):
                total = add(total, complex_mul(same[o][i], held[i]))
                total = add(total, complex_mul(cross[o][i], turned[i]))
            result.append(total)
        stage.append(result)
    for out_high in range(radix):
        coefs = [entry(high_gate, out_high, high) for high in range(radix)]
        ready = []
        for o in range(2):
            total = None
            for high in range(radix):
                total = add(total, complex_mul(coefs[high], stage[high][o]))
            mixed = None
            for step, coef in steps.items():
                mixed = add(mixed, complex_mul(coef, tuple(roll(v, -group * step) for v in total)))
            ready.append(mixed)
            rolled = tuple(roll(v, half) for v in mixed)
            at = out_high * radix + 2 * o
            send[at, :rows_hi] = jnp.where(first, mixed[0], rolled[1])
            send[at + 1, :rows_hi] = jnp.where(first, rolled[0], mixed[1])
        for take in range(radix):
            block = None
            for o in range(2):
                for c in range(2):
                    piece = roll(ready[o][c], (2 * o + c - take) * group)
                    block = piece if block is None else jnp.where(field == 2 * o + c, piece, block)
            send[out_high * radix + take, rows_hi:] = block

    pl.semaphore_wait(barrier, len(offsets))
    me = w * radix + n
    count = radix * radix
    seat = n * radix + w
    copies = []
    for at in range(count - 1):
        other = at + (at + count - seat) // count
        pw, pn = other % radix, other // radix
        copy = pltpu.make_async_remote_copy(
            src_ref=send.at[pw * radix + pn],
            dst_ref=recv.at[me],
            send_sem=send_sem.at[other],
            recv_sem=recv_sem.at[seat],
            device_id={"wide": pw, "narrow": pn},
            device_id_type=MESH,
        )
        copy.start()
        copies.append(copy)
    recv[me] = send[me]

    rest = list(range(start - 1)) + list(range(start + 2, total_pairs))
    rest = dict(zip(rest, merged_gates(planes, plan, rest)))
    low = kron_all([rest[pair] for pair in range(start - 2, -1, -1)], layers)
    block = jnp.concatenate(
        [jnp.concatenate([low[0], low[1]], axis=1), jnp.concatenate([-low[1], low[0]], axis=1)], axis=0
    )
    block = jnp.concatenate([jnp.concatenate([block] * radix, axis=0)] * radix, axis=1)
    down = lax.broadcasted_iota(jnp.int32, (LANES, LANES), 0)
    across = lax.broadcasted_iota(jnp.int32, (LANES, LANES), 1)
    grouped = jnp.where(down // (2 * group) == across // (2 * group), block, 0.0).T
    parts = [jnp.concatenate([jnp.concatenate([item] * radix, axis=0)] * radix, axis=1) for item in low]
    keep = (down[:half, :half] // group) == (across[:half, :half] // group)
    parts = [jnp.where(keep, item, 0.0) for item in parts]
    plain = jnp.concatenate(
        [jnp.concatenate([parts[0], parts[1]], axis=1), jnp.concatenate([-parts[1], parts[0]], axis=1)],
        axis=0,
    ).T
    for index, item in enumerate((plain, grouped)):
        lane_hi[index], lane_lo[index] = split(item)
    row_members = [rest[pair] for pair in range(total_pairs - 1, start + 1, -1)]
    for index, item in enumerate(kron_all(row_members, layers)):
        row_hi[index], row_lo[index] = split(item)

    for copy in copies:
        copy.wait_send()
    for at in range(count - 1):
        other = at + (at + count - seat) // count
        pw, pn = other % radix, other // radix
        pltpu.make_async_remote_copy(
            src_ref=send.at[me],
            dst_ref=recv.at[pw * radix + pn],
            send_sem=send_sem.at[other],
            recv_sem=recv_sem.at[other],
            device_id={"wide": pw, "narrow": pn},
            device_id_type=MESH,
        ).wait_recv()


def finish_kernel(radix, recv, lane_hi, lane_lo, row_hi, row_lo, out_hbm, marg_hbm, fin, marg, sems):
    rows_hi = recv.shape[1] // 2
    size = recv.shape[0] * rows_hi
    half = LANES // 2
    group = half // radix
    blocks = size // LANES
    rows = (row_hi[0], row_lo[0]), (row_hi[1], row_lo[1])

    def apply(which):
        held = split(recv[:, which * rows_hi : (which + 1) * rows_hi].reshape(size, LANES))
        turned = split(dot((lane_hi[which], lane_lo[which]), held, 1))
        return dot(turned, rows[0], 0), dot(turned, rows[1], 0)

    with_real, with_imag = apply(0)
    real = with_real[:half] - with_imag[half:]
    imag = with_real[half:] + with_imag[:half]
    for block in range(blocks):
        columns = slice(block * LANES, (block + 1) * LANES)
        fin[pl.ds(block * 2, half, stride=2 * blocks), :] = real[:, columns]
        fin[pl.ds(block * 2 + 1, half, stride=2 * blocks), :] = imag[:, columns]
    out_copy = pltpu.make_async_copy(fin, out_hbm, sems.at[0])
    out_copy.start()
    with_real, with_imag = apply(1)
    total = None
    for index in range(radix):
        at = 2 * group * index
        real = with_real[at : at + group] - with_imag[at + group : at + 2 * group]
        imag = with_real[at + group : at + 2 * group] + with_imag[at : at + group]
        term = real * real + imag * imag
        total = term if total is None else total + term
    for block in range(blocks):
        marg[pl.ds(block, group, stride=blocks), :] = total[:, block * LANES : (block + 1) * LANES]
    marg_copy = pltpu.make_async_copy(marg, marg_hbm, sems.at[1])
    marg_copy.start()
    out_copy.wait()
    marg_copy.wait()


def window_plan(wide_count, narrow_count, amplitudes, gates_shape):
    layers, pairs, radix = gates_shape[0], gates_shape[1], gates_shape[-1]
    high_bits = (wide_count * narrow_count).bit_length() - 1
    local_bits = amplitudes.bit_length() - 1
    total_bits = high_bits + local_bits
    if high_bits % 2 or local_bits % 2 or wide_count != radix or narrow_count != radix:
        return None
    if 2 * pairs != local_bits:
        return None
    offset = ((layers - 1) * high_bits) % total_bits
    start = offset // 2 - high_bits // 2
    if layers * radix > LANES or start < 2 or offset // 2 >= pairs or 2 * radix**start != LANES:
        return None
    rows_hi = radix ** (pairs - offset // 2)
    if rows_hi % 8:
        return None
    for which in range(total_bits // 2):
        if all((which - layer * (high_bits // 2)) % (total_bits // 2) >= pairs for layer in range(layers)):
            return None
    return (layers, pairs, high_bits // 2, total_bits // 2, start, radix), rows_hi


def merged_local(plan, rows_hi, state, gates):
    radix = plan[-1]
    amplitudes = state.shape[-1]
    rows = amplitudes // LANES
    count = radix * radix
    own = amplitudes // radix // LANES
    x = jnp.swapaxes(state.reshape(2, rows, LANES), 0, 1).reshape(2 * rows, LANES)
    g = jnp.transpose(gates, (1, 2, 3, 4, 0)).reshape(-1, radix, gates.shape[0])
    f32, bf16 = jnp.float32, jnp.bfloat16
    size = count * rows_hi
    shared = (
        pltpu.VMEM((count, 2 * rows_hi, LANES), f32),
        pltpu.VMEM((2, LANES, LANES), bf16),
        pltpu.VMEM((2, LANES, LANES), bf16),
        pltpu.VMEM((2, size, size), bf16),
        pltpu.VMEM((2, size, size), bf16),
    )
    held = pl.pallas_call(
        functools.partial(exchange_kernel, plan),
        out_shape=shared,
        in_specs=[pl.BlockSpec(memory_space=pltpu.HBM)] * 2,
        out_specs=[pl.BlockSpec(memory_space=pltpu.VMEM)] * len(shared),
        scratch_shapes=[
            pltpu.VMEM(x.shape, f32),
            pltpu.VMEM(g.shape, f32),
            pltpu.VMEM((count, 2 * rows_hi, LANES), f32),
            pltpu.SemaphoreType.DMA((2,)),
            pltpu.SemaphoreType.DMA((count,)),
            pltpu.SemaphoreType.DMA((count,)),
        ],
        compiler_params=pltpu.CompilerParams(
            collective_id=0, has_side_effects=True, vmem_limit_bytes=8 * 2**20
        ),
        name="exchange",
    )(
        pltpu.with_memory_space_constraint(x, pltpu.HBM),
        pltpu.with_memory_space_constraint(g, pltpu.HBM),
    )
    out, marg = pl.pallas_call(
        functools.partial(finish_kernel, radix),
        out_shape=(pltpu.HBM((2 * rows, LANES), f32), pltpu.HBM((own, LANES), f32)),
        in_specs=[pl.BlockSpec(memory_space=pltpu.VMEM)] * len(shared),
        out_specs=[pl.BlockSpec(memory_space=pltpu.HBM)] * 2,
        scratch_shapes=[
            pltpu.VMEM((2 * rows, LANES), f32),
            pltpu.VMEM((own, LANES), f32),
            pltpu.SemaphoreType.DMA((2,)),
        ],
        compiler_params=pltpu.CompilerParams(vmem_limit_bytes=8 * 2**20),
        name="finish",
    )(*held)
    final = jnp.swapaxes(out.reshape(rows, 2, LANES), 0, 1).reshape(1, 1, 2, amplitudes)
    return final, marg.reshape(1, -1)


def local(state, gates):
    wide_count = lax.axis_size("wide")
    narrow_count = lax.axis_size("narrow")
    amplitudes = state.shape[-1]
    found = window_plan(wide_count, narrow_count, amplitudes, gates.shape)
    if found is not None:
        return merged_local(*found, state, gates)
    flat = state.reshape(2, amplitudes)
    for layer_index in range(gates.shape[0]):
        if layer_index > 0:
            flat = rotate(flat, wide_count, narrow_count)
        flat = apply_layer(flat, gates[layer_index])
    prob = flat[0] * flat[0] + flat[1] * flat[1]
    marginal = lax.psum_scatter(prob, "narrow", scatter_dimension=0, tiled=True)
    return (flat.reshape(1, 1, 2, amplitudes), marginal.reshape(1, -1))


def solution(mesh):
    in_specs = (P(("slices", "wide"), "narrow", None, None), P())
    out_specs = (P(("slices", "wide"), "narrow", None, None), P(("slices", "wide"), "narrow"))
    return jax.shard_map(local, mesh=mesh, in_specs=in_specs, out_specs=out_specs, check_vma=False)
```

```python
import functools

import jax
import jax.numpy as jnp
from jax import lax
from jax.experimental import pallas as pl
from jax.experimental.pallas import tpu as pltpu
from jax.sharding import PartitionSpec as P


def kron_chain(members):
    real_part = members[0][0]
    imag_part = members[0][1]
    for member in members[1:]:
        other_real = member[0]
        other_imag = member[1]
        new_real = jnp.kron(real_part, other_real) - jnp.kron(imag_part, other_imag)
        new_imag = jnp.kron(real_part, other_imag) + jnp.kron(imag_part, other_real)
        real_part, imag_part = (new_real, new_imag)
    return (real_part, imag_part)


def rotate(flat, wide_count, narrow_count):
    devices = wide_count * narrow_count
    amplitudes = flat.shape[1]
    rest = amplitudes // devices
    blocks = flat.reshape(2, rest, devices)
    turned = jnp.swapaxes(blocks, 1, 2)
    moved = lax.all_to_all(turned, ("wide", "narrow"), split_axis=1, concat_axis=1, tiled=True)
    return moved.reshape(2, amplitudes)


def apply_layer(flat, layer_gates):
    amplitudes = flat.shape[1]
    pairs = layer_gates.shape[0]
    upper = amplitudes // 256
    low_real, low_imag = kron_chain([layer_gates[index] for index in range(3, -1, -1)])
    high_real, high_imag = kron_chain([layer_gates[index] for index in range(pairs - 1, 3, -1)])
    blocks = flat.reshape(2, upper, 256)
    real_rows = blocks[0]
    imag_rows = blocks[1]
    highest = lax.Precision.HIGHEST
    next_real = jnp.dot(real_rows, low_real.T, precision=highest) - jnp.dot(
        imag_rows, low_imag.T, precision=highest
    )
    next_imag = jnp.dot(real_rows, low_imag.T, precision=highest) + jnp.dot(
        imag_rows, low_real.T, precision=highest
    )
    final_real = jnp.dot(high_real, next_real, precision=highest) - jnp.dot(
        high_imag, next_imag, precision=highest
    )
    final_imag = jnp.dot(high_imag, next_real, precision=highest) + jnp.dot(
        high_real, next_imag, precision=highest
    )
    return jnp.stack([final_real, final_imag]).reshape(2, amplitudes)


MESH = pl.DeviceIdType.MESH
LANES = 128


def complex_mul(left, right):
    return (
        left[0] * right[0] - left[1] * right[1],
        left[0] * right[1] + left[1] * right[0],
    )


def merged_gates(planes, plan, which):
    layers, pairs, shift, total_pairs, _, radix = plan
    lane = lax.broadcasted_iota(jnp.int32, planes[0][0].shape, 1)
    down = lax.broadcasted_iota(jnp.int32, planes[0][0].shape, 0)
    unit = jnp.where(lane // layers == down, 1.0, 0.0)
    unit = (unit, jnp.zeros_like(unit))
    items = []
    for layer in range(layers):
        places = [(pair - layer * shift) % total_pairs for pair in which]
        chosen = [planes[place] if place < pairs else unit for place in places]
        items.append((tuple(jnp.stack([gate[c] for gate in chosen]) for c in range(2)), layer))
    while len(items) > 1:
        joined = []
        for at in range(0, len(items) - 1, 2):
            (early, last), (late, newest) = items[at], items[at + 1]
            total = None
            for row in range(radix):
                lane_at = row * layers + last
                term = complex_mul(
                    tuple(part[:, :, lane_at : lane_at + 1] for part in early),
                    tuple(part[:, row : row + 1, :] for part in late),
                )
                total = term if total is None else (total[0] + term[0], total[1] + term[1])
            joined.append((total, newest))
        if len(items) % 2:
            joined.append(items[-1])
        items = joined
    parts, last = items[0]
    return [(tuple(part[index] for part in parts), last) for index in range(len(which))]


def kron_all(members, layers):
    radix = members[0][0][0].shape[0]
    size = radix ** len(members)
    lane = lax.broadcasted_iota(jnp.int32, (1, size), 1)
    rows = None
    for place, (member, last) in enumerate(reversed(members)):
        field = (lane // radix**place) % radix
        wide = []
        for part in member:
            columns = [part[:, index * layers + last : index * layers + last + 1] for index in range(radix)]
            spread = jnp.broadcast_to(columns[-1], (radix, size))
            for index in range(radix - 1):
                spread = jnp.where(field == index, columns[index], spread)
            wide.append(spread)
        if rows is None:
            rows = tuple(wide)
            continue
        pieces = [
            complex_mul(tuple(part[index : index + 1, :] for part in wide), rows)
            for index in range(radix)
        ]
        rows = tuple(jnp.concatenate([piece[c] for piece in pieces], axis=0) for c in range(2))
    return rows


def split(value):
    high = value.astype(jnp.bfloat16)
    return high, (value - high.astype(jnp.float32)).astype(jnp.bfloat16)


def dot(left, right, contract):
    def one(a, b):
        return lax.dot_general(a, b, (((1,), (contract,)), ((), ())), preferred_element_type=jnp.float32)

    return one(left[0], right[0]) + (one(left[0], right[1]) + one(left[1], right[0]))


def exchange_kernel(plan, x_hbm, g_hbm, recv, lane_hi, lane_lo, row_hi, row_lo, x, g, send,
                    local_sem, send_sem, recv_sem):
    layers, pairs, shift, total_pairs, start, radix = plan
    w = lax.axis_index("wide")
    n = lax.axis_index("narrow")
    offsets = [(dw, dn) for dw in range(radix) for dn in range(radix) if dw or dn]

    def partner(dw, dn):
        return lax.rem(w + dw, radix), lax.rem(n + dn, radix)

    barrier = pltpu.get_barrier_semaphore()
    for dw, dn in offsets:
        pw, pn = partner(dw, dn)
        pl.semaphore_signal(barrier, inc=1, device_id={"wide": pw, "narrow": pn}, device_id_type=MESH)
    copy_g = pltpu.make_async_copy(g_hbm, g, local_sem.at[0])
    copy_x = pltpu.make_async_copy(x_hbm, x, local_sem.at[1])
    copy_g.start()
    copy_x.start()
    copy_g.wait()

    planes = []
    for index in range(pairs):
        plane = []
        for c in range(2):
            total = None
            for row in range(radix):
                tile = g[(index * 2 + c) * radix + row]
                tile = jnp.concatenate([tile, jnp.zeros((radix, LANES - layers), jnp.float32)], axis=1)
                tile = pltpu.roll(tile, row * layers, 1) if row else tile
                total = tile if total is None else total + tile
            plane.append(total)
        planes.append(tuple(plane))
    split_gate, low_gate, high_gate = merged_gates(planes, plan, range(start - 1, start + 2))

    half = LANES // 2
    group = half // radix
    rows_hi = send.shape[1] * radix // (2 * radix - 1)
    tail = rows_hi // radix
    shape = (rows_hi, LANES)
    lane = lax.broadcasted_iota(jnp.int32, shape, 1)
    first = lane < half
    field = (lane // group) % radix
    outer = lane // (2 * group)

    def entry(gate, row, column):
        lane_at = row * layers + gate[1]
        return tuple(
            jnp.broadcast_to(item[column : column + 1, lane_at : lane_at + 1], shape) for item in gate[0]
        )

    def both(gate, one, other):
        return tuple(jnp.where(first, a, b) for a, b in zip(entry(gate, *one), entry(gate, *other)))

    def add(total, term):
        return term if total is None else (total[0] + term[0], total[1] + term[1])

    def roll(value, amount):
        amount %= LANES
        return pltpu.roll(value, amount, 1) if amount else value

    steps = {}
    for row in range(radix):
        for column in range(radix):
            item = tuple(jnp.where(field == row, part, 0.0) for part in entry(split_gate, row, column))
            steps[column - row] = add(steps.get(column - row), item)

    copy_x.wait()
    same = [[both(low_gate, (2 * o, 2 * i), (2 * o + 1, 2 * i + 1)) for i in range(2)] for o in range(2)]
    cross = [[both(low_gate, (2 * o, 2 * i + 1), (2 * o + 1, 2 * i)) for i in range(2)] for o in range(2)]
    stage = []
    stride = 4 * radix
    for high in range(radix):
        held = []
        for i in range(2):
            held.append(tuple(x[pl.ds(high * 4 + i * 2 + c, rows_hi, stride=stride), :] for c in range(2)))
        turned = [tuple(roll(v, half) for v in pair) for pair in held]
        result = []
        for o in range(2):
            total = None
            for i in range(2):
                total = add(total, complex_mul(same[o][i], held[i]))
                total = add(total, complex_mul(cross[o][i], turned[i]))
            result.append(total)
        stage.append(result)
    for out_high in range(radix):
        coefs = [entry(high_gate, out_high, high) for high in range(radix)]
        ready = []
        for o in range(2):
            total = None
            for high in range(radix):
                total = add(total, complex_mul(coefs[high], stage[high][o]))
            mixed = None
            for step, coef in steps.items():
                mixed = add(mixed, complex_mul(coef, tuple(roll(v, -group * step) for v in total)))
            ready.append(mixed)
            rolled = tuple(roll(v, half) for v in mixed)
            at = out_high * radix + 2 * o
            send[at, :rows_hi] = jnp.where(first, mixed[0], rolled[1])
            send[at + 1, :rows_hi] = jnp.where(first, rolled[0], mixed[1])
        for take in range(radix):
            block = None
            for o in range(2):
                for c in range(2):
                    piece = roll(ready[o][c], (2 * o + c - take) * group)
                    block = piece if block is None else jnp.where(field == 2 * o + c, piece, block)
            spare = (take % 2) * 2 + take // 2
            if spare != radix - 1:
                block = jnp.where(outer == spare, roll(block, 2 * group * (spare + 1)), block)
            moved = [roll(block[rows_hi - tail :], -2 * group * (k + 1)) for k in range(radix - 1)]
            send[out_high * radix + take, rows_hi:] = jnp.where(
                outer[: rows_hi - tail] == radix - 1,
                jnp.concatenate(moved, axis=0),
                block[: rows_hi - tail],
            )

    pl.semaphore_wait(barrier, len(offsets))
    me = w * radix + n
    count = radix * radix
    seat = n * radix + w
    copies = []
    for at in range(count - 1):
        other = at + (at + count - seat) // count
        pw, pn = other % radix, other // radix
        copy = pltpu.make_async_remote_copy(
            src_ref=send.at[pw * radix + pn],
            dst_ref=recv.at[me],
            send_sem=send_sem.at[other],
            recv_sem=recv_sem.at[seat],
            device_id={"wide": pw, "narrow": pn},
            device_id_type=MESH,
        )
        copy.start()
        copies.append(copy)
    recv[me] = send[me]

    rest = list(range(start - 1)) + list(range(start + 2, total_pairs))
    rest = dict(zip(rest, merged_gates(planes, plan, rest)))
    low = kron_all([rest[pair] for pair in range(start - 2, -1, -1)], layers)
    block = jnp.concatenate(
        [jnp.concatenate([low[0], low[1]], axis=1), jnp.concatenate([-low[1], low[0]], axis=1)], axis=0
    )
    block = jnp.concatenate([jnp.concatenate([block] * radix, axis=0)] * radix, axis=1)
    down = lax.broadcasted_iota(jnp.int32, (LANES, LANES), 0)
    across = lax.broadcasted_iota(jnp.int32, (LANES, LANES), 1)
    grouped = jnp.where(down // (2 * group) == across // (2 * group), block, 0.0).T
    parts = [jnp.concatenate([jnp.concatenate([item] * radix, axis=0)] * radix, axis=1) for item in low]
    keep = (down[:half, :half] // group) == (across[:half, :half] // group)
    parts = [jnp.where(keep, item, 0.0) for item in parts]
    plain = jnp.concatenate(
        [jnp.concatenate([parts[0], parts[1]], axis=1), jnp.concatenate([-parts[1], parts[0]], axis=1)],
        axis=0,
    ).T
    for index, item in enumerate((plain, grouped)):
        lane_hi[index], lane_lo[index] = split(item)
    row_members = [rest[pair] for pair in range(total_pairs - 1, start + 1, -1)]
    for index, item in enumerate(kron_all(row_members, layers)):
        row_hi[index], row_lo[index] = split(item)

    for copy in copies:
        copy.wait_send()
    for at in range(count - 1):
        other = at + (at + count - seat) // count
        pw, pn = other % radix, other // radix
        pltpu.make_async_remote_copy(
            src_ref=send.at[me],
            dst_ref=recv.at[pw * radix + pn],
            send_sem=send_sem.at[other],
            recv_sem=recv_sem.at[other],
            device_id={"wide": pw, "narrow": pn},
            device_id_type=MESH,
        ).wait_recv()


def finish_kernel(radix, recv, lane_hi, lane_lo, row_hi, row_lo, out_hbm, marg_hbm, fin, prob, marg, sems):
    rows_hi = recv.shape[1] * radix // (2 * radix - 1)
    tail = rows_hi // radix
    size = recv.shape[0] * rows_hi
    half = LANES // 2
    group = half // radix
    blocks = size // LANES
    rows = (row_hi[0], row_lo[0]), (row_hi[1], row_lo[1])

    def apply(which, value, keep):
        held = split(value.reshape(size, LANES))
        turned = dot((lane_hi[which], lane_lo[which]), held, 1)
        turned = split(turned[:keep])
        return dot(turned, rows[0], 0), dot(turned, rows[1], 0)

    with_real, with_imag = apply(0, recv[:, :rows_hi], LANES)
    real = with_real[:half] - with_imag[half:]
    imag = with_real[half:] + with_imag[:half]
    for block in range(blocks):
        columns = slice(block * LANES, (block + 1) * LANES)
        fin[pl.ds(block * 2, half, stride=2 * blocks), :] = real[:, columns]
        fin[pl.ds(block * 2 + 1, half, stride=2 * blocks), :] = imag[:, columns]
    out_copy = pltpu.make_async_copy(fin, out_hbm, sems.at[0])
    out_copy.start()
    density = real * real + imag * imag
    for index in range(radix):
        prob[index] = density[index * group : (index + 1) * group]
    packed = recv[:, rows_hi:]
    outer = lax.broadcasted_iota(jnp.int32, (1, tail, LANES), 2) // (2 * group)
    last = None
    for index in range(radix - 1):
        piece = packed[:, index * tail : (index + 1) * tail]
        piece = pltpu.roll(piece, 2 * group * (index + 1), 2)
        last = piece if last is None else jnp.where(outer == index, piece, last)
    wide = jnp.concatenate([packed, last], axis=1)
    with_real, with_imag = apply(1, wide, LANES - 2 * group)
    total = prob[lax.axis_index("narrow")]
    for index in range(radix - 1):
        at = 2 * group * index
        real = with_real[at : at + group] - with_imag[at + group : at + 2 * group]
        imag = with_real[at + group : at + 2 * group] + with_imag[at : at + group]
        term = real * real + imag * imag
        total = total + term
    for block in range(blocks):
        marg[pl.ds(block, group, stride=blocks), :] = total[:, block * LANES : (block + 1) * LANES]
    marg_copy = pltpu.make_async_copy(marg, marg_hbm, sems.at[1])
    marg_copy.start()
    out_copy.wait()
    marg_copy.wait()


def window_plan(wide_count, narrow_count, amplitudes, gates_shape):
    layers, pairs, radix = gates_shape[0], gates_shape[1], gates_shape[-1]
    high_bits = (wide_count * narrow_count).bit_length() - 1
    local_bits = amplitudes.bit_length() - 1
    total_bits = high_bits + local_bits
    if high_bits % 2 or local_bits % 2 or wide_count != radix or narrow_count != radix:
        return None
    if 2 * pairs != local_bits:
        return None
    offset = ((layers - 1) * high_bits) % total_bits
    start = offset // 2 - high_bits // 2
    if layers * radix > LANES or start < 2 or offset // 2 >= pairs or 2 * radix**start != LANES:
        return None
    rows_hi = radix ** (pairs - offset // 2)
    if rows_hi % 8:
        return None
    for which in range(total_bits // 2):
        if all((which - layer * (high_bits // 2)) % (total_bits // 2) >= pairs for layer in range(layers)):
            return None
    return (layers, pairs, high_bits // 2, total_bits // 2, start, radix), rows_hi


def merged_local(plan, rows_hi, state, gates):
    radix = plan[-1]
    amplitudes = state.shape[-1]
    rows = amplitudes // LANES
    count = radix * radix
    own = amplitudes // radix // LANES
    x = jnp.swapaxes(state.reshape(2, rows, LANES), 0, 1).reshape(2 * rows, LANES)
    g = jnp.transpose(gates, (1, 2, 3, 4, 0)).reshape(-1, radix, gates.shape[0])
    f32, bf16 = jnp.float32, jnp.bfloat16
    size = count * rows_hi
    message = 2 * rows_hi - rows_hi // radix
    shared = (
        pltpu.VMEM((count, message, LANES), f32),
        pltpu.VMEM((2, LANES, LANES), bf16),
        pltpu.VMEM((2, LANES, LANES), bf16),
        pltpu.VMEM((2, size, size), bf16),
        pltpu.VMEM((2, size, size), bf16),
    )
    held = pl.pallas_call(
        functools.partial(exchange_kernel, plan),
        out_shape=shared,
        in_specs=[pl.BlockSpec(memory_space=pltpu.HBM)] * 2,
        out_specs=[pl.BlockSpec(memory_space=pltpu.VMEM)] * len(shared),
        scratch_shapes=[
            pltpu.VMEM(x.shape, f32),
            pltpu.VMEM(g.shape, f32),
            pltpu.VMEM((count, message, LANES), f32),
            pltpu.SemaphoreType.DMA((2,)),
            pltpu.SemaphoreType.DMA((count,)),
            pltpu.SemaphoreType.DMA((count,)),
        ],
        compiler_params=pltpu.CompilerParams(
            collective_id=0, has_side_effects=True, vmem_limit_bytes=8 * 2**20
        ),
        name="exchange",
    )(
        pltpu.with_memory_space_constraint(x, pltpu.HBM),
        pltpu.with_memory_space_constraint(g, pltpu.HBM),
    )
    out, marg = pl.pallas_call(
        functools.partial(finish_kernel, radix),
        out_shape=(pltpu.HBM((2 * rows, LANES), f32), pltpu.HBM((own, LANES), f32)),
        in_specs=[pl.BlockSpec(memory_space=pltpu.VMEM)] * len(shared),
        out_specs=[pl.BlockSpec(memory_space=pltpu.HBM)] * 2,
        scratch_shapes=[
            pltpu.VMEM((2 * rows, LANES), f32),
            pltpu.VMEM((radix, LANES // 2 // radix, size), f32),
            pltpu.VMEM((own, LANES), f32),
            pltpu.SemaphoreType.DMA((2,)),
        ],
        compiler_params=pltpu.CompilerParams(vmem_limit_bytes=8 * 2**20),
        name="finish",
    )(*held)
    final = jnp.swapaxes(out.reshape(rows, 2, LANES), 0, 1).reshape(1, 1, 2, amplitudes)
    return final, marg.reshape(1, -1)


def local(state, gates):
    wide_count = lax.axis_size("wide")
    narrow_count = lax.axis_size("narrow")
    amplitudes = state.shape[-1]
    found = window_plan(wide_count, narrow_count, amplitudes, gates.shape)
    if found is not None:
        return merged_local(*found, state, gates)
    flat = state.reshape(2, amplitudes)
    for layer_index in range(gates.shape[0]):
        if layer_index > 0:
            flat = rotate(flat, wide_count, narrow_count)
        flat = apply_layer(flat, gates[layer_index])
    prob = flat[0] * flat[0] + flat[1] * flat[1]
    marginal = lax.psum_scatter(prob, "narrow", scatter_dimension=0, tiled=True)
    return (flat.reshape(1, 1, 2, amplitudes), marginal.reshape(1, -1))


def solution(mesh):
    in_specs = (P(("slices", "wide"), "narrow", None, None), P())
    out_specs = (P(("slices", "wide"), "narrow", None, None), P(("slices", "wide"), "narrow"))
    return jax.shard_map(local, mesh=mesh, in_specs=in_specs, out_specs=out_specs, check_vma=False)
```

```python
import functools

import jax
import jax.numpy as jnp
from jax import lax
from jax.experimental import pallas as pl
from jax.experimental.pallas import tpu as pltpu
from jax.sharding import PartitionSpec as P


def kron_chain(members):
    real_part = members[0][0]
    imag_part = members[0][1]
    for member in members[1:]:
        other_real = member[0]
        other_imag = member[1]
        new_real = jnp.kron(real_part, other_real) - jnp.kron(imag_part, other_imag)
        new_imag = jnp.kron(real_part, other_imag) + jnp.kron(imag_part, other_real)
        real_part, imag_part = (new_real, new_imag)
    return (real_part, imag_part)


def rotate(flat, wide_count, narrow_count):
    devices = wide_count * narrow_count
    amplitudes = flat.shape[1]
    rest = amplitudes // devices
    blocks = flat.reshape(2, rest, devices)
    turned = jnp.swapaxes(blocks, 1, 2)
    moved = lax.all_to_all(turned, ("wide", "narrow"), split_axis=1, concat_axis=1, tiled=True)
    return moved.reshape(2, amplitudes)


def apply_layer(flat, layer_gates):
    amplitudes = flat.shape[1]
    pairs = layer_gates.shape[0]
    upper = amplitudes // 256
    low_real, low_imag = kron_chain([layer_gates[index] for index in range(3, -1, -1)])
    high_real, high_imag = kron_chain([layer_gates[index] for index in range(pairs - 1, 3, -1)])
    blocks = flat.reshape(2, upper, 256)
    real_rows = blocks[0]
    imag_rows = blocks[1]
    highest = lax.Precision.HIGHEST
    next_real = jnp.dot(real_rows, low_real.T, precision=highest) - jnp.dot(
        imag_rows, low_imag.T, precision=highest
    )
    next_imag = jnp.dot(real_rows, low_imag.T, precision=highest) + jnp.dot(
        imag_rows, low_real.T, precision=highest
    )
    final_real = jnp.dot(high_real, next_real, precision=highest) - jnp.dot(
        high_imag, next_imag, precision=highest
    )
    final_imag = jnp.dot(high_imag, next_real, precision=highest) + jnp.dot(
        high_real, next_imag, precision=highest
    )
    return jnp.stack([final_real, final_imag]).reshape(2, amplitudes)


MESH = pl.DeviceIdType.MESH
LANES = 128


def complex_mul(left, right):
    return (
        left[0] * right[0] - left[1] * right[1],
        left[0] * right[1] + left[1] * right[0],
    )


def merged_gates(planes, plan, which):
    layers, pairs, shift, total_pairs, _, radix = plan
    lane = lax.broadcasted_iota(jnp.int32, planes[0][0].shape, 1)
    down = lax.broadcasted_iota(jnp.int32, planes[0][0].shape, 0)
    unit = jnp.where(lane // layers == down, 1.0, 0.0)
    unit = (unit, jnp.zeros_like(unit))
    items = []
    for layer in range(layers):
        places = [(pair - layer * shift) % total_pairs for pair in which]
        chosen = [planes[place] if place < pairs else unit for place in places]
        items.append((tuple(jnp.stack([gate[c] for gate in chosen]) for c in range(2)), layer))
    while len(items) > 1:
        joined = []
        for at in range(0, len(items) - 1, 2):
            (early, last), (late, newest) = items[at], items[at + 1]
            total = None
            for row in range(radix):
                lane_at = row * layers + last
                term = complex_mul(
                    tuple(part[:, :, lane_at : lane_at + 1] for part in early),
                    tuple(part[:, row : row + 1, :] for part in late),
                )
                total = term if total is None else (total[0] + term[0], total[1] + term[1])
            joined.append((total, newest))
        if len(items) % 2:
            joined.append(items[-1])
        items = joined
    parts, last = items[0]
    return [(tuple(part[index] for part in parts), last) for index in range(len(which))]


def kron_all(members, layers):
    radix = members[0][0][0].shape[0]
    size = radix ** len(members)
    lane = lax.broadcasted_iota(jnp.int32, (1, size), 1)
    rows = None
    for place, (member, last) in enumerate(reversed(members)):
        field = (lane // radix**place) % radix
        wide = []
        for part in member:
            columns = [part[:, index * layers + last : index * layers + last + 1] for index in range(radix)]
            spread = jnp.broadcast_to(columns[-1], (radix, size))
            for index in range(radix - 1):
                spread = jnp.where(field == index, columns[index], spread)
            wide.append(spread)
        if rows is None:
            rows = tuple(wide)
            continue
        pieces = [
            complex_mul(tuple(part[index : index + 1, :] for part in wide), rows)
            for index in range(radix)
        ]
        rows = tuple(jnp.concatenate([piece[c] for piece in pieces], axis=0) for c in range(2))
    return rows


def split(value):
    high = value.astype(jnp.bfloat16)
    return high, (value - high.astype(jnp.float32)).astype(jnp.bfloat16)


def dot(left, right, contract):
    def one(a, b):
        return lax.dot_general(a, b, (((1,), (contract,)), ((), ())), preferred_element_type=jnp.float32)

    return one(left[0], right[0]) + (one(left[0], right[1]) + one(left[1], right[0]))


def exchange_kernel(plan, x_hbm, g_hbm, recv, lane_hi, lane_lo, row_hi, row_lo, x, g, send,
                    local_sem, send_sem, recv_sem):
    layers, pairs, shift, total_pairs, start, radix = plan
    w = lax.axis_index("wide")
    n = lax.axis_index("narrow")
    offsets = [(dw, dn) for dw in range(radix) for dn in range(radix) if dw or dn]

    def partner(dw, dn):
        return lax.rem(w + dw, radix), lax.rem(n + dn, radix)

    barrier = pltpu.get_barrier_semaphore()
    copy_g = pltpu.make_async_copy(g_hbm, g, local_sem.at[0])
    copy_x = pltpu.make_async_copy(x_hbm, x, local_sem.at[1])
    copy_g.start()
    copy_x.start()
    for dw, dn in offsets:
        pw, pn = partner(dw, dn)
        pl.semaphore_signal(barrier, inc=1, device_id={"wide": pw, "narrow": pn}, device_id_type=MESH)
    copy_g.wait()

    planes = []
    for index in range(pairs):
        plane = []
        for c in range(2):
            total = None
            for row in range(radix):
                tile = g[(index * 2 + c) * radix + row]
                tile = jnp.concatenate([tile, jnp.zeros((radix, LANES - layers), jnp.float32)], axis=1)
                tile = pltpu.roll(tile, row * layers, 1) if row else tile
                total = tile if total is None else total + tile
            plane.append(total)
        planes.append(tuple(plane))
    split_gate, low_gate, high_gate = merged_gates(planes, plan, range(start - 1, start + 2))

    half = LANES // 2
    group = half // radix
    rows_hi = send.shape[1] * radix // (2 * radix - 1)
    tail = rows_hi // radix
    shape = (rows_hi, LANES)
    lane = lax.broadcasted_iota(jnp.int32, shape, 1)
    first = lane < half
    field = (lane // group) % radix
    outer = lane // (2 * group)

    def entry(gate, row, column):
        lane_at = row * layers + gate[1]
        return tuple(
            jnp.broadcast_to(item[column : column + 1, lane_at : lane_at + 1], shape) for item in gate[0]
        )

    def both(gate, one, other):
        return tuple(jnp.where(first, a, b) for a, b in zip(entry(gate, *one), entry(gate, *other)))

    def add(total, term):
        return term if total is None else (total[0] + term[0], total[1] + term[1])

    def roll(value, amount):
        amount %= LANES
        return pltpu.roll(value, amount, 1) if amount else value

    steps = {}
    for row in range(radix):
        for column in range(radix):
            item = tuple(jnp.where(field == row, part, 0.0) for part in entry(split_gate, row, column))
            steps[column - row] = add(steps.get(column - row), item)

    copy_x.wait()
    same = [[both(low_gate, (2 * o, 2 * i), (2 * o + 1, 2 * i + 1)) for i in range(2)] for o in range(2)]
    cross = [[both(low_gate, (2 * o, 2 * i + 1), (2 * o + 1, 2 * i)) for i in range(2)] for o in range(2)]
    stage = []
    stride = 4 * radix
    for high in range(radix):
        held = []
        for i in range(2):
            held.append(tuple(x[pl.ds(high * 4 + i * 2 + c, rows_hi, stride=stride), :] for c in range(2)))
        turned = [tuple(roll(v, half) for v in pair) for pair in held]
        result = []
        for o in range(2):
            total = None
            for i in range(2):
                total = add(total, complex_mul(same[o][i], held[i]))
                total = add(total, complex_mul(cross[o][i], turned[i]))
            result.append(total)
        stage.append(result)
    for out_high in range(radix):
        coefs = [entry(high_gate, out_high, high) for high in range(radix)]
        ready = []
        for o in range(2):
            total = None
            for high in range(radix):
                total = add(total, complex_mul(coefs[high], stage[high][o]))
            mixed = None
            for step, coef in steps.items():
                mixed = add(mixed, complex_mul(coef, tuple(roll(v, -group * step) for v in total)))
            ready.append(mixed)
            rolled = tuple(roll(v, half) for v in mixed)
            at = out_high * radix + 2 * o
            send[at, :rows_hi] = jnp.where(first, mixed[0], rolled[1])
            send[at + 1, :rows_hi] = jnp.where(first, rolled[0], mixed[1])
        for take in range(radix):
            block = None
            for o in range(2):
                for c in range(2):
                    piece = roll(ready[o][c], (2 * o + c - take) * group)
                    block = piece if block is None else jnp.where(field == 2 * o + c, piece, block)
            spare = (take % 2) * 2 + take // 2
            if spare != radix - 1:
                block = jnp.where(outer == spare, roll(block, 2 * group * (spare + 1)), block)
            moved = [roll(block[rows_hi - tail :], -2 * group * (k + 1)) for k in range(radix - 1)]
            send[out_high * radix + take, rows_hi:] = jnp.where(
                outer[: rows_hi - tail] == radix - 1,
                jnp.concatenate(moved, axis=0),
                block[: rows_hi - tail],
            )

    pl.semaphore_wait(barrier, len(offsets))
    me = w * radix + n
    count = radix * radix
    seat = ((radix - n) % radix) * radix + w
    copies = []
    for at in range(count - 1):
        other = at + (at + count - seat) // count
        pw, pn = other % radix, (radix - other // radix) % radix
        copy = pltpu.make_async_remote_copy(
            src_ref=send.at[pw * radix + pn],
            dst_ref=recv.at[me],
            send_sem=send_sem.at[other],
            recv_sem=recv_sem.at[seat],
            device_id={"wide": pw, "narrow": pn},
            device_id_type=MESH,
        )
        copy.start()
        copies.append(copy)
    recv[me] = send[me]

    rest = list(range(start - 1)) + list(range(start + 2, total_pairs))
    rest = dict(zip(rest, merged_gates(planes, plan, rest)))
    low = kron_all([rest[pair] for pair in range(start - 2, -1, -1)], layers)
    block = jnp.concatenate(
        [jnp.concatenate([low[0], low[1]], axis=1), jnp.concatenate([-low[1], low[0]], axis=1)], axis=0
    )
    block = jnp.concatenate([jnp.concatenate([block] * radix, axis=0)] * radix, axis=1)
    down = lax.broadcasted_iota(jnp.int32, (LANES, LANES), 0)
    across = lax.broadcasted_iota(jnp.int32, (LANES, LANES), 1)
    grouped = jnp.where(down // (2 * group) == across // (2 * group), block, 0.0).T
    parts = [jnp.concatenate([jnp.concatenate([item] * radix, axis=0)] * radix, axis=1) for item in low]
    keep = (down[:half, :half] // group) == (across[:half, :half] // group)
    parts = [jnp.where(keep, item, 0.0) for item in parts]
    plain = jnp.concatenate(
        [jnp.concatenate([parts[0], parts[1]], axis=1), jnp.concatenate([-parts[1], parts[0]], axis=1)],
        axis=0,
    ).T
    for index, item in enumerate((plain, grouped)):
        lane_hi[index], lane_lo[index] = split(item)
    row_members = [rest[pair] for pair in range(total_pairs - 1, start + 1, -1)]
    for index, item in enumerate(kron_all(row_members, layers)):
        row_hi[index], row_lo[index] = split(item)

    for copy in copies:
        copy.wait_send()
    for at in range(count - 1):
        other = at + (at + count - seat) // count
        pw, pn = other % radix, (radix - other // radix) % radix
        pltpu.make_async_remote_copy(
            src_ref=send.at[me],
            dst_ref=recv.at[pw * radix + pn],
            send_sem=send_sem.at[other],
            recv_sem=recv_sem.at[other],
            device_id={"wide": pw, "narrow": pn},
            device_id_type=MESH,
        ).wait_recv()


def finish_kernel(radix, recv, lane_hi, lane_lo, row_hi, row_lo, out_hbm, marg_hbm, fin, prob, marg, sems):
    rows_hi = recv.shape[1] * radix // (2 * radix - 1)
    tail = rows_hi // radix
    size = recv.shape[0] * rows_hi
    half = LANES // 2
    group = half // radix
    blocks = size // LANES
    rows = (row_hi[0], row_lo[0]), (row_hi[1], row_lo[1])

    def apply(which, value, keep):
        held = split(value.reshape(size, LANES))
        turned = dot((lane_hi[which], lane_lo[which]), held, 1)
        turned = split(turned[:keep])
        return dot(turned, rows[0], 0), dot(turned, rows[1], 0)

    with_real, with_imag = apply(0, recv[:, :rows_hi], LANES)
    real = with_real[:half] - with_imag[half:]
    imag = with_real[half:] + with_imag[:half]
    for block in range(blocks):
        columns = slice(block * LANES, (block + 1) * LANES)
        fin[pl.ds(block * 2, half, stride=2 * blocks), :] = real[:, columns]
        fin[pl.ds(block * 2 + 1, half, stride=2 * blocks), :] = imag[:, columns]
    out_copy = pltpu.make_async_copy(fin, out_hbm, sems.at[0])
    out_copy.start()
    density = real * real + imag * imag
    for index in range(radix):
        prob[index] = density[index * group : (index + 1) * group]
    packed = recv[:, rows_hi:]
    outer = lax.broadcasted_iota(jnp.int32, (1, tail, LANES), 2) // (2 * group)
    last = None
    for index in range(radix - 1):
        piece = packed[:, index * tail : (index + 1) * tail]
        piece = pltpu.roll(piece, 2 * group * (index + 1), 2)
        last = piece if last is None else jnp.where(outer == index, piece, last)
    wide = jnp.concatenate([packed, last], axis=1)
    with_real, with_imag = apply(1, wide, LANES - 2 * group)
    total = prob[lax.axis_index("narrow")]
    for index in range(radix - 1):
        at = 2 * group * index
        real = with_real[at : at + group] - with_imag[at + group : at + 2 * group]
        imag = with_real[at + group : at + 2 * group] + with_imag[at : at + group]
        term = real * real + imag * imag
        total = total + term
    for block in range(blocks):
        marg[pl.ds(block, group, stride=blocks), :] = total[:, block * LANES : (block + 1) * LANES]
    marg_copy = pltpu.make_async_copy(marg, marg_hbm, sems.at[1])
    marg_copy.start()
    out_copy.wait()
    marg_copy.wait()


def window_plan(wide_count, narrow_count, amplitudes, gates_shape):
    layers, pairs, radix = gates_shape[0], gates_shape[1], gates_shape[-1]
    high_bits = (wide_count * narrow_count).bit_length() - 1
    local_bits = amplitudes.bit_length() - 1
    total_bits = high_bits + local_bits
    if high_bits % 2 or local_bits % 2 or wide_count != radix or narrow_count != radix:
        return None
    if 2 * pairs != local_bits:
        return None
    offset = ((layers - 1) * high_bits) % total_bits
    start = offset // 2 - high_bits // 2
    if layers * radix > LANES or start < 2 or offset // 2 >= pairs or 2 * radix**start != LANES:
        return None
    rows_hi = radix ** (pairs - offset // 2)
    if rows_hi % 8:
        return None
    for which in range(total_bits // 2):
        if all((which - layer * (high_bits // 2)) % (total_bits // 2) >= pairs for layer in range(layers)):
            return None
    return (layers, pairs, high_bits // 2, total_bits // 2, start, radix), rows_hi


def merged_local(plan, rows_hi, state, gates):
    radix = plan[-1]
    amplitudes = state.shape[-1]
    rows = amplitudes // LANES
    count = radix * radix
    own = amplitudes // radix // LANES
    x = jnp.swapaxes(state.reshape(2, rows, LANES), 0, 1).reshape(2 * rows, LANES)
    g = jnp.transpose(gates, (1, 2, 3, 4, 0)).reshape(-1, radix, gates.shape[0])
    f32, bf16 = jnp.float32, jnp.bfloat16
    size = count * rows_hi
    message = 2 * rows_hi - rows_hi // radix
    shared = (
        pltpu.VMEM((count, message, LANES), f32),
        pltpu.VMEM((2, LANES, LANES), bf16),
        pltpu.VMEM((2, LANES, LANES), bf16),
        pltpu.VMEM((2, size, size), bf16),
        pltpu.VMEM((2, size, size), bf16),
    )
    held = pl.pallas_call(
        functools.partial(exchange_kernel, plan),
        out_shape=shared,
        in_specs=[pl.BlockSpec(memory_space=pltpu.HBM)] * 2,
        out_specs=[pl.BlockSpec(memory_space=pltpu.VMEM)] * len(shared),
        scratch_shapes=[
            pltpu.VMEM(x.shape, f32),
            pltpu.VMEM(g.shape, f32),
            pltpu.VMEM((count, message, LANES), f32),
            pltpu.SemaphoreType.DMA((2,)),
            pltpu.SemaphoreType.DMA((count,)),
            pltpu.SemaphoreType.DMA((count,)),
        ],
        compiler_params=pltpu.CompilerParams(
            collective_id=0, has_side_effects=True, vmem_limit_bytes=8 * 2**20
        ),
        name="exchange",
    )(
        pltpu.with_memory_space_constraint(x, pltpu.HBM),
        pltpu.with_memory_space_constraint(g, pltpu.HBM),
    )
    out, marg = pl.pallas_call(
        functools.partial(finish_kernel, radix),
        out_shape=(pltpu.HBM((2 * rows, LANES), f32), pltpu.HBM((own, LANES), f32)),
        in_specs=[pl.BlockSpec(memory_space=pltpu.VMEM)] * len(shared),
        out_specs=[pl.BlockSpec(memory_space=pltpu.HBM)] * 2,
        scratch_shapes=[
            pltpu.VMEM((2 * rows, LANES), f32),
            pltpu.VMEM((radix, LANES // 2 // radix, size), f32),
            pltpu.VMEM((own, LANES), f32),
            pltpu.SemaphoreType.DMA((2,)),
        ],
        compiler_params=pltpu.CompilerParams(vmem_limit_bytes=8 * 2**20),
        name="finish",
    )(*held)
    final = jnp.swapaxes(out.reshape(rows, 2, LANES), 0, 1).reshape(1, 1, 2, amplitudes)
    return final, marg.reshape(1, -1)


def local(state, gates):
    wide_count = lax.axis_size("wide")
    narrow_count = lax.axis_size("narrow")
    amplitudes = state.shape[-1]
    found = window_plan(wide_count, narrow_count, amplitudes, gates.shape)
    if found is not None:
        return merged_local(*found, state, gates)
    flat = state.reshape(2, amplitudes)
    for layer_index in range(gates.shape[0]):
        if layer_index > 0:
            flat = rotate(flat, wide_count, narrow_count)
        flat = apply_layer(flat, gates[layer_index])
    prob = flat[0] * flat[0] + flat[1] * flat[1]
    marginal = lax.psum_scatter(prob, "narrow", scatter_dimension=0, tiled=True)
    return (flat.reshape(1, 1, 2, amplitudes), marginal.reshape(1, -1))


def solution(mesh):
    in_specs = (P(("slices", "wide"), "narrow", None, None), P())
    out_specs = (P(("slices", "wide"), "narrow", None, None), P(("slices", "wide"), "narrow"))
    return jax.shard_map(local, mesh=mesh, in_specs=in_specs, out_specs=out_specs, check_vma=False)
```
